8 devices in a mesh: dp: 1 (over z), sp: 8 (over y, x, core).
Axes of the slice: x: 2, y: 2, z: 1, core: 2. Of those that a mesh axis runs over, the one named last changes fastest.
Arguments:
- tokens: bfloat16 [16384, 768], P(('dp', 'sp'))
- grad_out: bfloat16 [16384, 768], P(('dp', 'sp'))
- ln_gain: float32 [768], replicated
- ln_bias: float32 [768], replicated
- w_qkv: bfloat16 [768, 2304], replicated
- w_out: bfloat16 [768, 768], replicated
- temperature: float32 [16], replicated
Outputs:
- output 1: bfloat16 [16384, 768], P(('dp', 'sp'))
- output 2: bfloat16 [16384, 768], P(('dp', 'sp'))
- output 3: float32 [768, 2304], P(('dp', 'sp'))
- output 4: float32 [768, 768], P(('dp', 'sp'))
- output 5: float32 [768], P('dp')
- output 6: float32 [768], P('dp')
- output 7: float32 [16], P('dp')
All inputs are finite; a program needn't handle non-finite values.
Results may differ from the reference program's by a relative error of at most 0.0014325.
Values are sent between devices in bfloat16 or wider.
A program may use at most 1 GiB of HBM per device.

```python
import jax
import jax.numpy as jnp
from jax import lax

SEQ_LEN = 16384
MODEL_DIM = 768
NUM_HEADS = 16

HEAD_DIM = MODEL_DIM // NUM_HEADS


def setup_inputs(seed: int = 0, part: int = 0) -> dict:
    part_keys = jax.random.split(jax.random.fold_in(jax.random.key(seed), part), 4)
    shared_keys = jax.random.split(jax.random.key(seed + 1), 5)
    position = (jnp.arange(SEQ_LEN, dtype=jnp.float32) + 0.5) / SEQ_LEN
    wave_basis = jnp.cos(jnp.pi * position[:, None] * jnp.arange(1, 5, dtype=jnp.float32)[None, :])
    x_pattern = jnp.dot(wave_basis, jax.random.normal(part_keys[0], (4, MODEL_DIM), jnp.float32))
    tokens = jax.random.normal(part_keys[1], (SEQ_LEN, MODEL_DIM), jnp.float32) + x_pattern
    dy_pattern = jnp.dot(wave_basis, jax.random.normal(part_keys[2], (4, MODEL_DIM), jnp.float32))
    grad_out = jax.random.normal(part_keys[3], (SEQ_LEN, MODEL_DIM), jnp.float32) + 0.5 * dy_pattern
    w_scale = MODEL_DIM ** -0.5
    return {
        'tokens': tokens.astype(jnp.bfloat16),
        'grad_out': grad_out.astype(jnp.bfloat16),
        'ln_gain': 1.0 + 0.3 * jax.random.normal(shared_keys[0], (MODEL_DIM,), jnp.float32),
        'ln_bias': 0.3 * jax.random.normal(shared_keys[1], (MODEL_DIM,), jnp.float32),
        'w_qkv': (w_scale * jax.random.normal(shared_keys[2], (MODEL_DIM, 3 * MODEL_DIM), jnp.float32)).astype(jnp.bfloat16),
        'w_out': (w_scale * jax.random.normal(shared_keys[3], (MODEL_DIM, MODEL_DIM), jnp.float32)).astype(jnp.bfloat16),
        'temperature': jax.random.uniform(shared_keys[4], (NUM_HEADS,), jnp.float32, 2.5, 6.5),
    }


def layer_norm(x_f32, ln_gain, ln_bias):
    row_mean = jnp.mean(x_f32, axis=-1, keepdims=True)
    centered = x_f32 - row_mean
    row_var = jnp.mean(centered * centered, axis=-1, keepdims=True)
    return centered * lax.rsqrt(row_var + 1e-6) * ln_gain + ln_bias


def attn_probs(gram_sum, q_sq, k_sq, temperature):
    cosine = gram_sum / (jnp.sqrt(q_sq)[..., :, None] * jnp.sqrt(k_sq)[..., None, :])
    return jax.nn.softmax(temperature[..., None, None] * cosine, axis=-1)


def reference(tokens, grad_out, ln_gain, ln_bias, w_qkv, w_out, temperature):
    x_f32 = tokens.astype(jnp.float32)
    ln_value, ln_vjp = jax.vjp(layer_norm, x_f32, ln_gain, ln_bias)
    normed = ln_value.astype(jnp.bfloat16)
    qkv_act = jnp.dot(normed, w_qkv, preferred_element_type=jnp.float32).astype(jnp.bfloat16)
    qkv_heads = qkv_act.astype(jnp.float32).reshape(SEQ_LEN, 3, NUM_HEADS, HEAD_DIM)
    q_heads = qkv_heads[:, 0]
    k_heads = qkv_heads[:, 1]
    v_heads = qkv_heads[:, 2]
    gram_sum = jnp.einsum('nhi,nhj->hij', q_heads, k_heads)
    q_sq = jnp.sum(q_heads * q_heads, axis=0)
    k_sq = jnp.sum(k_heads * k_heads, axis=0)
    attn_f32, probs_vjp = jax.vjp(attn_probs, gram_sum, q_sq, k_sq, temperature)
    attn_weights = attn_f32.astype(jnp.bfloat16).astype(jnp.float32)
    attn_out = jnp.einsum('nhj,hij->nhi', v_heads, attn_weights).astype(jnp.bfloat16).reshape(SEQ_LEN, MODEL_DIM)
    out_tokens = (x_f32 + jnp.dot(attn_out, w_out, preferred_element_type=jnp.float32)).astype(jnp.bfloat16)

    grad_w_out = jnp.dot(attn_out.T, grad_out, preferred_element_type=jnp.float32)
    d_attn = jnp.dot(grad_out, w_out.T, preferred_element_type=jnp.float32).astype(jnp.bfloat16)
    d_heads = d_attn.astype(jnp.float32).reshape(SEQ_LEN, NUM_HEADS, HEAD_DIM)
    d_probs = jnp.einsum('nhi,nhj->hij', d_heads, v_heads)
    d_gram, d_qsq, d_ksq, grad_temperature = probs_vjp(d_probs)
    d_gram_bf = d_gram.astype(jnp.bfloat16).astype(jnp.float32)
    d_q = jnp.einsum('hij,nhj->nhi', d_gram_bf, k_heads) + 2.0 * q_heads * d_qsq
    d_k = jnp.einsum('hij,nhi->nhj', d_gram_bf, q_heads) + 2.0 * k_heads * d_ksq
    d_v = jnp.einsum('hij,nhi->nhj', attn_weights, d_heads)
    d_qkv = jnp.stack([d_q, d_k, d_v], axis=1).astype(jnp.bfloat16).reshape(SEQ_LEN, 3 * MODEL_DIM)
    grad_w_qkv = jnp.dot(normed.T, d_qkv, preferred_element_type=jnp.float32)
    d_normed = jnp.dot(d_qkv, w_qkv.T, preferred_element_type=jnp.float32)
    d_x, grad_gain, grad_bias = ln_vjp(d_normed)
    grad_tokens = (grad_out.astype(jnp.float32) + d_x).astype(jnp.bfloat16)
    return (out_tokens, grad_tokens, grad_w_qkv, grad_w_out, grad_gain, grad_bias, grad_temperature)
```

```python
import jax
import jax.numpy as jnp
from jax import lax
from jax.experimental import pallas as pl
from jax.experimental.pallas import tpu as pltpu
from jax.sharding import PartitionSpec as P

F32 = jnp.float32
BF16 = jnp.bfloat16
MESH = pl.DeviceIdType.MESH

ROWS = 2048
WIDTH = 768
HEADS = 16
HD = 48
GW = 384
GH = 8
BLK = 512
NBLK = ROWS // BLK
LNR = 32
PAY = 400
HALF = PAY // 2
SHARD = 96
CHUNKS = 8


def dot(a, b, ca, cb):
    return lax.dot_general(a, b, (((ca,), (cb,)), ((), ())), preferred_element_type=F32)


def kernel(temp_ref, gain_ref, bias_ref, x_hbm, dy_hbm, wqkv_hbm, wout_hbm,
           out_hbm, gtok_hbm, gwqkv_hbm, gwout_hbm, gb_out, dtemp_out,
           x_v, dy_v, u_v, ut_v, qkv_v, do_v, ot_v, w_v, wo_v,
           gm_v, sq_v, bd_v, dsq_v, row_v, pay_v, ar1, ar2, ar3, sum_v,
           gw_v, r1, r2, r3, fin_v, du_v, gb_v, gbs_v, gbr_v,
           in_sem, w_sem, out_sem, fin_sem,
           ar_send, ar_recv, s1_send, s1_recv, s2_send, s2_recv, s3_send, s3_recv, gb_send, gb_recv):
    dp = lax.axis_index('dp')
    me = lax.axis_index('sp')
    core = me % 2
    cx = (me // 2) % 2
    cy = me // 4
    partner = me + 1 - 2 * core
    xn = me + 2 - 4 * cx
    yn = me + 4 - 8 * cy
    first = xn + core * (yn - xn)
    second = yn + core * (xn - yn)
    ca = cx + core * (cy - cx)
    cb = cy + core * (cx - cy)

    def chip(a, b):
        return a * (1 + core) + b * (2 - core)

    def dev(i):
        return (dp, i)

    def remote(src, dst, ss, rs, to):
        return pltpu.make_async_remote_copy(src_ref=src, dst_ref=dst, send_sem=ss, recv_sem=rs,
                                            device_id=dev(to), device_id_type=MESH)

    barrier = pltpu.get_barrier_semaphore()
    for peer in (partner, xn, yn):
        pl.semaphore_signal(barrier, inc=1, device_id=dev(peer), device_id_type=MESH)

    def w_copy(g, p):
        return pltpu.make_async_copy(wqkv_hbm.at[:, pl.ds(p * WIDTH + g * GW, GW)],
                                     w_v.at[g, :, pl.ds(p * GW, GW)], w_sem.at[3 * g + p])

    wo_copy = pltpu.make_async_copy(wout_hbm, wo_v, w_sem.at[6])

    def x_copy(b):
        rows = pl.ds(b * BLK, BLK)
        return pltpu.make_async_copy(x_hbm.at[rows], x_v.at[rows], in_sem.at[0, b])

    def dy_copy(b):
        rows = pl.ds(b * BLK, BLK)
        return pltpu.make_async_copy(dy_hbm.at[rows], dy_v.at[rows], in_sem.at[1, b])

    x_copy(0).start()
    for p in range(3):
        w_copy(0, p).start()
    dy_copy(0).start()
    wo_copy.start()
    for b in range(1, NBLK):
        x_copy(b).start()
        dy_copy(b).start()
    for p in range(3):
        w_copy(1, p).start()

    gain = gain_ref[...]
    bias = bias_ref[...]

    def normed_rows(r0):
        xf = x_v[pl.ds(r0, LNR), :].astype(F32)
        c = xf - jnp.mean(xf, axis=-1, keepdims=True)
        rstd = lax.rsqrt(jnp.mean(c * c, axis=-1, keepdims=True) + 1e-6)
        return c * rstd, rstd

    def sumsq(v):
        vf = v.astype(F32)
        return jnp.sum((vf * vf).reshape(BLK // 8, 8, GW), axis=0)

    def project(g, b, with_ln):
        r0 = pl.multiple_of(b * BLK, BLK)
        rows = pl.ds(r0, BLK)
        if with_ln:
            for i in range(BLK // LNR):
                xhat, _ = normed_rows(r0 + i * LNR)
                u_v[pl.ds(r0 + i * LNR, LNR), :] = (xhat * gain + bias).astype(BF16)
        u = u_v[rows, :]
        if with_ln:
            ut_v[:, rows] = u.T
            do_v[rows, :] = dot(dy_v[rows, :], wo_v[...], 1, 1).astype(BF16)
        qkv = dot(u, w_v[g], 1, 0).astype(BF16)
        qkv_v[g, rows, :] = qkv
        sq_v[g, 0] += sumsq(qkv[:, :GW])
        sq_v[g, 1] += sumsq(qkv[:, GW:2 * GW])

    def grams(g):
        gm_v[0] = dot(qkv_v[g, :, :GW], qkv_v[g, :, GW:2 * GW], 0, 0)
        gm_v[1] = dot(do_v[:, g * GW:(g + 1) * GW], qkv_v[g, :, 2 * GW:], 0, 0)
        lane = lax.broadcasted_iota(jnp.int32, (HD, 128), 1)
        pay = pay_v.at[g]
        for h in range(GH):
            lo = HD * h // 128 * 128
            hi = min(lo + 256, GW)
            off = HD * h - lo
            a = gm_v[0, HD * h:HD * (h + 1), lo:hi]
            d = gm_v[1, HD * h:HD * (h + 1), lo:hi]
            n = hi - lo
            if off:
                a = pltpu.roll(a, n - off, 1)
            a = a[:, :128]
            s = (64 - off) % n
            if s:
                d = pltpu.roll(d, s, 1)
            d = d[:, :128]
            both = jnp.where(lane < HD, a, jnp.where((lane >= 64) & (lane < 64 + HD), d, 0.0))
            pay[HD * h:HD * (h + 1), :] = both
        pay[GW:PAY, :] = jnp.zeros((PAY - GW, 128), F32)
        for p in range(2):
            row = jnp.sum(sq_v[g, p], axis=0, keepdims=True)
            for c in range(3):
                r = GW + 3 * p + c
                pay[r:r + 1, :] = row[:, 128 * c:128 * (c + 1)]

    mine = pl.ds(pl.multiple_of(core * HALF, 8), HALF)
    theirs = pl.ds(pl.multiple_of((1 - core) * HALF, 8), HALF)

    held = {}

    def ar_step(g, k):
        if k == 1:
            held[g, 0].wait()
            pay_v[g, mine, :] = ar1[g] + pay_v[g, mine, :]
        elif k == 2:
            held[g, 1].wait()
            pay_v[g, mine, :] = ar2[g] + pay_v[g, mine, :]
        elif k == 3:
            held[g, 2].wait()
            sum_v[g, mine, :] = ar3[g] + pay_v[g, mine, :]
        elif k == 4:
            held[g, 3].wait()
            return
        if k == 0:
            src, dst, to = pay_v.at[g, theirs], ar1.at[g], partner
        elif k == 1:
            src, dst, to = pay_v.at[g, mine], ar2.at[g], first
        elif k == 2:
            src, dst, to = pay_v.at[g, mine], ar3.at[g], second
        else:
            src, dst, to = sum_v.at[g, mine], sum_v.at[g, mine], partner
        held[g, k] = remote(src, dst, ar_send.at[g, k], ar_recv.at[g, k], to)
        held[g, k].start()

    def spread(rows3, h):
        wide = jnp.broadcast_to(rows3, (8, GW))
        if h:
            wide = pltpu.roll(wide, GW - HD * h, 1)
        return wide[:1, :128]

    def place(v, h):
        wide = jnp.concatenate([v, jnp.zeros((v.shape[0], GW - 128), v.dtype)], axis=1)
        return pltpu.roll(wide, HD * h, 1) if h else wide

    def small(g):
        sqrow = jnp.concatenate([sum_v[g, GW + c:GW + c + 1, :] for c in range(3)], axis=1)
        skrow = jnp.concatenate([sum_v[g, GW + 3 + c:GW + 4 + c, :] for c in range(3)], axis=1)
        for c in range(3):
            row_v[128 * c:128 * (c + 1), :] = jnp.broadcast_to(sqrow[:, 128 * c:128 * (c + 1)], (128, 128)).T
        lane = lax.broadcasted_iota(jnp.int32, (HD, 128), 1)
        ok = lane < HD
        dsk = jnp.zeros((8, GW), F32)
        for h in range(GH):
            hr = slice(HD * h, HD * (h + 1))
            both = sum_v[g, hr, :]
            gram = jnp.where(ok, both, 0.0)
            da = jnp.where(ok, pltpu.roll(both, 64, 1), 0.0)
            sqc = row_v[hr, :]
            skh = jnp.broadcast_to(spread(skrow, h), (HD, 128))
            skh = jnp.where(ok, skh, 1.0)
            den = jnp.sqrt(sqc) * jnp.sqrt(skh)
            cosine = gram / den
            t = temp_ref[g * GH + h]
            logit = jnp.where(ok, t * cosine, -jnp.inf)
            top = jnp.max(logit, axis=1, keepdims=True)
            e = jnp.where(ok, jnp.exp(logit - top), 0.0)
            a = e / jnp.sum(e, axis=1, keepdims=True)
            ds = a * (da - jnp.sum(a * da, axis=1, keepdims=True))
            dtemp_out[g * GH + h:g * GH + h + 1, :] = jnp.broadcast_to(
                jnp.sum(jnp.sum(ds * cosine, axis=1, keepdims=True), axis=0, keepdims=True), (1, 128))
            dcos = t * ds
            dg = dcos / den
            w = dcos * cosine
            row_v[hr, :] = -jnp.sum(w, axis=1, keepdims=True) / sqc
            dskh = jnp.sum(w, axis=0, keepdims=True) / skh[:1]
            dsk = dsk + place(jnp.broadcast_to(-dskh, (8, 128)), h)
            bd_v[g, 0, hr, :] = place(a, h).astype(BF16)
            bd_v[g, 1, hr, :] = place(dg, h).astype(BF16)
        dsq_v[g, 8:16, :] = dsk
        dsq_v[g, 0:8, :] = jnp.concatenate(
            [row_v[128 * c:128 * (c + 1), :].T[:8] for c in range(3)], axis=1)

    def heads(g, b):
        rows = pl.ds(pl.multiple_of(b * BLK, BLK), BLK)
        cols = slice(g * GW, (g + 1) * GW)
        attn = bd_v[g, 0]
        dgram = bd_v[g, 1]
        dsq = dsq_v[g, 0:1, :]
        dsk = dsq_v[g, 8:9, :]
        q = qkv_v[g, rows, :GW]
        k = qkv_v[g, rows, GW:2 * GW]
        v = qkv_v[g, rows, 2 * GW:]
        do = do_v[rows, cols]
        o = dot(v, attn, 1, 1).astype(BF16)
        dq = (dot(k, dgram, 1, 1) + q.astype(F32) * dsq).astype(BF16)
        dk = (dot(q, dgram, 1, 0) + k.astype(F32) * dsk).astype(BF16)
        dv = dot(do, attn, 1, 0).astype(BF16)
        qkv_v[g, rows, :GW] = dq
        qkv_v[g, rows, GW:2 * GW] = dk
        qkv_v[g, rows, 2 * GW:] = dv
        do_v[rows, cols] = o
        ot_v[cols, rows] = o.T

    def gw_chunk(ch):
        def half(m, carry):
            mr = pl.ds(pl.multiple_of(m * GW, GW), GW)
            if ch < 6:
                g, p = divmod(ch, 3)
                res = dot(ut_v[mr, :], qkv_v[g, :, p * GW:(p + 1) * GW], 1, 0)
            else:
                res = dot(ot_v[mr, :], dy_v[:, (ch - 6) * GW:(ch - 5) * GW], 1, 0)
            gw_v[ch, pl.ds(2 * m, 2)] = res.reshape(2, 2, SHARD, GW)
            return carry
        lax.fori_loop(0, 2, half, 0)

    def s1(ch):
        c = remote(gw_v.at[ch, :, 1 - core], r1.at[ch], s1_send.at[ch], s1_recv.at[ch], partner)
        c.start()
        held['s1', ch] = c

    def s2(ch):
        held['s1', ch].wait()
        for a, b in ((1 - ca, 1 - cb), (1 - ca, cb), (ca, 1 - cb), (ca, cb)):
            i = chip(a, b)
            r1[ch, i] += gw_v[ch, i, core]
        for n, b in ((0, 1 - cb), (1, cb)):
            c = remote(r1.at[ch, chip(1 - ca, b)], r2.at[ch, b], s2_send.at[ch, b], s2_recv.at[ch, b], first)
            c.start()
            held['s2', ch, n] = c

    def s3(ch):
        held['s2', ch, 0].wait()
        held['s2', ch, 1].wait()
        for b in (1 - cb, cb):
            r2[ch, b] += r1[ch, chip(ca, b)]
        c = remote(r2.at[ch, 1 - cb], r3.at[ch], s3_send.at[ch], s3_recv.at[ch], second)
        c.start()
        held['s3', ch] = c

    def s4(ch):
        held['s3', ch].wait()
        fin_v[ch] = r3[ch] + r2[ch, cb]
        if ch < 6:
            g, p = divmod(ch, 3)
            dst = gwqkv_hbm.at[:, pl.ds(p * WIDTH + g * GW, GW)]
        else:
            dst = gwout_hbm.at[:, pl.ds((ch - 6) * GW, GW)]
        c = pltpu.make_async_copy(fin_v.at[ch], dst, fin_sem.at[ch])
        c.start()
        held['fin', ch] = c

    gsum = (jnp.zeros((8, WIDTH), F32), jnp.zeros((8, WIDTH), F32))

    def final_block(b):
        r0 = pl.multiple_of(b * BLK, BLK)
        rows = pl.ds(r0, BLK)
        du_v[...] = dot(qkv_v[0, rows, :], w_v[0], 1, 1) + dot(qkv_v[1, rows, :], w_v[1], 1, 1)
        do_v[rows, :] = (x_v[rows, :].astype(F32) + dot(do_v[rows, :], wo_v[...], 1, 0)).astype(BF16)
        pltpu.make_async_copy(do_v.at[rows], out_hbm.at[rows], out_sem.at[0, b]).start()
        dgain = jnp.zeros((8, WIDTH), F32)
        dbias = jnp.zeros((8, WIDTH), F32)
        for i in range(BLK // LNR):
            sub = pl.ds(r0 + i * LNR, LNR)
            xhat, rstd = normed_rows(r0 + i * LNR)
            du = du_v[i * LNR:(i + 1) * LNR, :]
            dgain = dgain + jnp.sum((du * xhat).reshape(LNR // 8, 8, WIDTH), axis=0)
            dbias = dbias + jnp.sum(du.reshape(LNR // 8, 8, WIDTH), axis=0)
            dxh = du * gain
            m1 = jnp.mean(dxh, axis=-1, keepdims=True)
            m2 = jnp.mean(dxh * xhat, axis=-1, keepdims=True)
            dx = rstd * (dxh - m1 - xhat * m2)
            x_v[sub, :] = (dy_v[sub, :].astype(F32) + dx).astype(BF16)
        gb_v[0] += dgain
        gb_v[1] += dbias
        pltpu.make_async_copy(x_v.at[rows], gtok_hbm.at[rows], out_sem.at[1, b]).start()

    def gb_start(k):
        to = (partner, first, second)[k]
        c = remote(gbs_v.at[k], gbr_v.at[k], gb_send.at[k], gb_recv.at[k], to)
        c.start()
        held['gb', k] = c

    def gb_next(k):
        held['gb', k].wait()
        total = gbs_v[k] + gbr_v[k]
        if k < 2:
            gbs_v[k + 1] = total
            gb_start(k + 1)
        else:
            gb_out[...] = total

    sq_v[...] = jnp.zeros_like(sq_v)
    gb_v[...] = jnp.zeros_like(gb_v)
    for p in range(3):
        w_copy(0, p).wait()
    wo_copy.wait()

    def first_pass(b, carry):
        x_copy(b).wait()
        dy_copy(b).wait()
        project(0, b, True)
        return carry
    lax.fori_loop(0, NBLK, first_pass, 0)
    grams(0)
    pl.semaphore_wait(barrier, 3)
    ar_step(0, 0)
    for p in range(3):
        w_copy(1, p).wait()

    def loop(f, lo, hi):
        def body(b, carry):
            f(b)
            return carry
        lax.fori_loop(lo, hi, body, 0)

    loop(lambda b: project(1, b, False), 0, 1)
    ar_step(0, 1)
    loop(lambda b: project(1, b, False), 1, 3)
    ar_step(0, 2)
    loop(lambda b: project(1, b, False), 3, 4)
    grams(1)
    ar_step(1, 0)
    ar_step(0, 3)
    ar_step(1, 1)
    ar_step(0, 4)
    small(0)
    ar_step(1, 2)
    loop(lambda b: heads(0, b), 0, NBLK)
    ar_step(1, 3)
    gw_chunk(0)
    s1(0)
    gw_chunk(1)
    s1(1)
    s2(0)
    gw_chunk(2)
    s1(2)
    s2(1)
    ar_step(1, 4)
    small(1)
    s2(2)
    loop(lambda b: heads(1, b), 0, NBLK)
    s3(0)
    gw_chunk(3)
    s1(3)
    s3(1)
    gw_chunk(4)
    s1(4)
    s2(3)
    gw_chunk(5)
    s1(5)
    s2(4)
    s3(2)
    gw_chunk(6)
    s1(6)
    s2(5)
    gw_chunk(7)
    s1(7)
    s2(6)
    s3(3)
    final_block(0)
    s2(7)
    s3(4)
    final_block(1)
    s3(5)
    final_block(2)
    s3(6)
    final_block(3)
    gbs_v[0] = jnp.concatenate([jnp.sum(gb_v[i], axis=0, keepdims=True) for i in range(2)]
                               + [jnp.zeros((6, WIDTH), F32)], axis=0)
    gb_start(0)
    for ch in range(0, 4):
        s4(ch)
    gb_next(0)
    for ch in range(4, 6):
        s4(ch)
    s3(7)
    gb_next(1)
    s4(6)
    gb_next(2)
    s4(7)
    for b in range(NBLK):
        rows = pl.ds(b * BLK, BLK)
        pltpu.make_async_copy(do_v.at[rows], out_hbm.at[rows], out_sem.at[0, b]).wait()
        pltpu.make_async_copy(x_v.at[rows], gtok_hbm.at[rows], out_sem.at[1, b]).wait()
    for ch in range(CHUNKS):
        held['fin', ch].wait()


def block_step(x, dy, ln_gain, ln_bias, w_qkv, w_out, temperature):
    any_spec = pl.BlockSpec(memory_space=pl.ANY)
    vmem = pl.BlockSpec(memory_space=pltpu.VMEM)
    dma = pltpu.SemaphoreType.DMA
    return pl.pallas_call(
        kernel,
        out_shape=(
            jax.ShapeDtypeStruct((ROWS, WIDTH), BF16),
            jax.ShapeDtypeStruct((ROWS, WIDTH), BF16),
            jax.ShapeDtypeStruct((SHARD, 3 * WIDTH), F32),
            jax.ShapeDtypeStruct((SHARD, WIDTH), F32),
            jax.ShapeDtypeStruct((8, WIDTH), F32),
            jax.ShapeDtypeStruct((HEADS, 128), F32),
        ),
        in_specs=[pl.BlockSpec(memory_space=pltpu.SMEM), vmem, vmem, any_spec, any_spec, any_spec, any_spec],
        out_specs=(any_spec, any_spec, any_spec, any_spec, vmem, vmem),
        scratch_shapes=[
            pltpu.VMEM((ROWS, WIDTH), BF16),
            pltpu.VMEM((ROWS, WIDTH), BF16),
            pltpu.VMEM((ROWS, WIDTH), BF16),
            pltpu.VMEM((WIDTH, ROWS), BF16),
            pltpu.VMEM((2, ROWS, 3 * GW), BF16),
            pltpu.VMEM((ROWS, WIDTH), BF16),
            pltpu.VMEM((WIDTH, ROWS), BF16),
            pltpu.VMEM((2, WIDTH, 3 * GW), BF16),
            pltpu.VMEM((WIDTH, WIDTH), BF16),
            pltpu.VMEM((2, GW, GW), F32),
            pltpu.VMEM((2, 2, 8, GW), F32),
            pltpu.VMEM((2, 2, GW, GW), BF16),
            pltpu.VMEM((2, 16, GW), F32),
            pltpu.VMEM((GW, 128), F32),
            pltpu.VMEM((2, PAY, 128), F32),
            pltpu.VMEM((2, HALF, 128), F32),
            pltpu.VMEM((2, HALF, 128), F32),
            pltpu.VMEM((2, HALF, 128), F32),
            pltpu.VMEM((2, PAY, 128), F32),
            pltpu.VMEM((CHUNKS, 4, 2, SHARD, GW), F32),
            pltpu.VMEM((CHUNKS, 4, SHARD, GW), F32),
            pltpu.VMEM((CHUNKS, 2, SHARD, GW), F32),
            pltpu.VMEM((CHUNKS, SHARD, GW), F32),
            pltpu.VMEM((CHUNKS, SHARD, GW), F32),
            pltpu.VMEM((BLK, WIDTH), F32),
            pltpu.VMEM((2, 8, WIDTH), F32),
            pltpu.VMEM((3, 8, WIDTH), F32),
            pltpu.VMEM((3, 8, WIDTH), F32),
            dma((2, NBLK)), dma((7,)), dma((2, NBLK)), dma((CHUNKS,)),
            dma((2, 4)), dma((2, 4)),
            dma((CHUNKS,)), dma((CHUNKS,)),
            dma((CHUNKS, 2)), dma((CHUNKS, 2)),
            dma((CHUNKS,)), dma((CHUNKS,)),
            dma((3,)), dma((3,)),
        ],
        compiler_params=pltpu.CompilerParams(
            collective_id=0, has_side_effects=True, vmem_limit_bytes=67043328),
    )(temperature, ln_gain.reshape(1, WIDTH), ln_bias.reshape(1, WIDTH), x, dy, w_qkv, w_out)


def solution(mesh):
    row_spec = P(('dp', 'sp'), None)
    part_spec = P('dp')
    full_spec = P()

    def local_step(x, dy, ln_gain, ln_bias, w_qkv, w_out, temperature):
        out, gtok, gwqkv, gwout, gb, dtemp = block_step(x, dy, ln_gain, ln_bias, w_qkv, w_out, temperature)
        return out, gtok, gwqkv, gwout, gb[0], gb[1], dtemp[:, 0]

    return jax.shard_map(local_step, mesh=mesh,
                         in_specs=(row_spec, row_spec, full_spec, full_spec, full_spec, full_spec, full_spec),
                         out_specs=(row_spec, row_spec, row_spec, row_spec, part_spec, part_spec, part_spec),
                         check_vma=False)
```

```python
import jax
import jax.numpy as jnp
from jax import lax
from jax.experimental import pallas as pl
from jax.experimental.pallas import tpu as pltpu
from jax.sharding import PartitionSpec as P

F32 = jnp.float32
BF16 = jnp.bfloat16
MESH = pl.DeviceIdType.MESH

ROWS = 2048
WIDTH = 768
HEADS = 16
HD = 48
GW = 384
GH = 8
BLK = 512
NBLK = ROWS // BLK
LNR = 32
PAIR = 192
TOT = 2304
MSG = (208, 192, 400)
MSG0 = (0, 208, 400)
SHARD = 96
CHUNKS = 8


def dot(a, b, ca, cb):
    return lax.dot_general(a, b, (((ca,), (cb,)), ((), ())), preferred_element_type=F32)


def kernel(temp_ref, gain_ref, bias_ref, x_hbm, dy_hbm, wqkv_hbm, wout_hbm,
           x_v, do_v, gwq_out, gwo_out, gb_out, dtemp_out,
           dy_v, u_v, ut_v, qkv_v, ot_v, w_v, wo_v,
           gm_v, sq_v, a_v, bd_v, dsq_v, row_v, pay_v, ar1, ar2, ar3, sum_v,
           gw_v, r1, r2, r3, du_v, gb_v, gbs_v, gbr_v,
           in_sem, w_sem,
           ar_send, ar_recv, s1_send, s1_recv, s2_send, s2_recv, s3_send, s3_recv, gb_send, gb_recv):
    dp = lax.axis_index('dp')
    me = lax.axis_index('sp')
    core = me % 2
    cx = (me // 2) % 2
    cy = me // 4
    partner = me + 1 - 2 * core
    xn = me + 2 - 4 * cx
    yn = me + 4 - 8 * cy
    first = xn + core * (yn - xn)
    second = yn + core * (xn - yn)
    ca = cx + core * (cy - cx)
    cb = cy + core * (cx - cy)

    def chip(a, b):
        return a * (1 + core) + b * (2 - core)

    def dev(i):
        return (dp, i)

    def remote(src, dst, ss, rs, to):
        return pltpu.make_async_remote_copy(src_ref=src, dst_ref=dst, send_sem=ss, recv_sem=rs,
                                            device_id=dev(to), device_id_type=MESH)

    barrier = pltpu.get_barrier_semaphore()
    for peer in (partner, xn, yn):
        pl.semaphore_signal(barrier, inc=1, device_id=dev(peer), device_id_type=MESH)

    def w_copy(g, p):
        return pltpu.make_async_copy(wqkv_hbm.at[:, pl.ds(p * WIDTH + g * GW, GW)],
                                     w_v.at[:, pl.ds((3 * g + p) * GW, GW)], w_sem.at[3 * g + p])

    wo_copy = pltpu.make_async_copy(wout_hbm, wo_v, w_sem.at[6])

    def x_copy(b):
        rows = pl.ds(b * BLK, BLK)
        return pltpu.make_async_copy(x_hbm.at[rows], x_v.at[rows], in_sem.at[0, b])

    def dy_copy(b):
        rows = pl.ds(b * BLK, BLK)
        return pltpu.make_async_copy(dy_hbm.at[rows], dy_v.at[rows], in_sem.at[1, b])

    x_copy(0).start()
    w_copy(0, 0).start()
    w_copy(0, 1).start()
    for b in range(1, NBLK):
        x_copy(b).start()
    w_copy(0, 2).start()
    wo_copy.start()
    for b in range(NBLK):
        dy_copy(b).start()
    for p in range(3):
        w_copy(1, p).start()

    gain = gain_ref[...].reshape(1, WIDTH)
    bias = bias_ref[...].reshape(1, WIDTH)

    def loop(f):
        def body(b, carry):
            f(b)
            return carry
        lax.fori_loop(0, NBLK, body, 0)

    def block(b):
        return pl.ds(pl.multiple_of(b * BLK, BLK), BLK)

    def normed_rows(r0):
        xf = x_v[pl.ds(r0, LNR), :].astype(F32)
        c = xf - jnp.mean(xf, axis=-1, keepdims=True)
        rstd = lax.rsqrt(jnp.mean(c * c, axis=-1, keepdims=True) + 1e-6)
        return c * rstd, rstd

    def norm_block(b):
        for i in range(BLK // LNR):
            r0 = b * BLK + i * LNR
            xhat, _ = normed_rows(r0)
            u_v[r0:r0 + LNR, :] = (xhat * gain + bias).astype(BF16)

    def sumsq(v):
        vf = v.astype(F32)
        return jnp.sum((vf * vf).reshape(BLK // 8, 8, GW), axis=0)

    def project(g, lo, hi, rows):
        res = dot(u_v[rows, :], w_v[:, (3 * g + lo) * GW:(3 * g + hi) * GW], 1, 0).astype(BF16)
        qkv_v[rows, (3 * g + lo) * GW:(3 * g + hi) * GW] = res
        if lo == 0:
            sq_v[g, 0] += sumsq(res[:, :GW])
            sq_v[g, 1] += sumsq(res[:, GW:2 * GW])

    def values_and_do(b):
        rows = block(b)
        project(0, 2, 3, rows)
        do_v[rows, :] = dot(dy_v[rows, :], wo_v[...], 1, 1).astype(BF16)
        ut_v[:, rows] = u_v[rows, :].T

    def pack(res, base):
        gm_v[...] = res
        lane = lax.broadcasted_iota(jnp.int32, (HD, 128), 1)

        def piece(h, to):
            lo = HD * h // 128 * 128
            hi = min(lo + 256, GW)
            v = gm_v[HD * h:HD * (h + 1), lo:hi]
            s = (to - (HD * h - lo)) % (hi - lo)
            if s:
                v = pltpu.roll(v, s, 1)
            return v[:, :128]
        for p in range(GH // 2):
            a = piece(2 * p, 0)
            d = piece(2 * p + 1, 64)
            both = jnp.where(lane < HD, a, jnp.where((lane >= 64) & (lane < 64 + HD), d, 0.0))
            pay_v[base + HD * p:base + HD * (p + 1), :] = both

    def gram(g, base):
        pack(dot(qkv_v[:, 3 * g * GW:(3 * g + 1) * GW], qkv_v[:, (3 * g + 1) * GW:(3 * g + 2) * GW], 0, 0), base)
        r0 = base + PAIR
        pay_v[r0:r0 + 16, :] = jnp.zeros((16, 128), F32)
        for p in range(2):
            row = jnp.sum(sq_v[g, p], axis=0, keepdims=True)
            for c in range(3):
                pay_v[r0 + 3 * p + c:r0 + 3 * p + c + 1, :] = row[:, 128 * c:128 * (c + 1)]

    def dgram(g, base):
        pack(dot(do_v[:, g * GW:(g + 1) * GW], qkv_v[:, (3 * g + 2) * GW:(3 * g + 3) * GW], 0, 0), base)

    held = {}

    def ar(m, k):
        half = MSG[m] // 2
        mine = pl.ds(pl.multiple_of(MSG0[m] + core * half, 8), half)
        theirs = pl.ds(pl.multiple_of(MSG0[m] + (1 - core) * half, 8), half)
        slot = pl.ds(MSG0[m] // 2, half)
        if k:
            held[m, k - 1].wait()
        if k == 1:
            pay_v[mine, :] = ar1[slot, :] + pay_v[mine, :]
        elif k == 2:
            pay_v[mine, :] = ar2[slot, :] + pay_v[mine, :]
        elif k == 3:
            sum_v[mine, :] = ar3[slot, :] + pay_v[mine, :]
        elif k == 4:
            return
        if k == 0:
            src, dst, to = pay_v.at[theirs], ar1.at[slot], partner
        elif k == 1:
            src, dst, to = pay_v.at[mine], ar2.at[slot], first
        elif k == 2:
            src, dst, to = pay_v.at[mine], ar3.at[slot], second
        else:
            src, dst, to = sum_v.at[mine], sum_v.at[mine], partner
        held[m, k] = remote(src, dst, ar_send.at[m, k], ar_recv.at[m, k], to)
        held[m, k].start()

    lane48 = lax.broadcasted_iota(jnp.int32, (HD, 128), 1)
    ok = lane48 < HD

    def place(v, h):
        wide = jnp.concatenate([v, jnp.zeros((v.shape[0], GW - 128), v.dtype)], axis=1)
        return pltpu.roll(wide, HD * h, 1) if h else wide

    def head_block(base, h):
        both = sum_v[base + HD * (h // 2):base + HD * (h // 2 + 1), :]
        if h % 2:
            both = pltpu.roll(both, 64, 1)
        return jnp.where(ok, both, 0.0)

    def attn(g, base):
        r0 = base + PAIR
        sqrow = jnp.concatenate([sum_v[r0 + c:r0 + c + 1, :] for c in range(3)], axis=1)
        skrow = jnp.concatenate([sum_v[r0 + 3 + c:r0 + 4 + c, :] for c in range(3)], axis=1)
        skwide = jnp.broadcast_to(skrow, (8, GW))
        for c in range(3):
            row_v[128 * c:128 * (c + 1), :] = jnp.broadcast_to(sqrow[:, 128 * c:128 * (c + 1)], (128, 128)).T
        for h in range(GH):
            hr = slice(HD * h, HD * (h + 1))
            skh = pltpu.roll(skwide, GW - HD * h, 1) if h else skwide
            skh = jnp.where(ok, jnp.broadcast_to(skh[:1, :128], (HD, 128)), 1.0)
            den = jnp.sqrt(row_v[hr, :]) * jnp.sqrt(skh)
            cosine = head_block(base, h) / den
            logit = jnp.where(ok, temp_ref[g * GH + h] * cosine, -jnp.inf)
            e = jnp.where(ok, jnp.exp(logit - jnp.max(logit, axis=1, keepdims=True)), 0.0)
            a = e / jnp.sum(e, axis=1, keepdims=True)
            a_v[0, hr, :] = a
            a_v[1, hr, :] = cosine
            a_v[2, hr, :] = den
            bd_v[0, hr, :] = place(a, h).astype(BF16)

    def attn_vjp(g, gbase, dbase):
        r0 = gbase + PAIR
        skrow = jnp.concatenate([sum_v[r0 + 3 + c:r0 + 4 + c, :] for c in range(3)], axis=1)
        dsk = jnp.zeros((8, GW), F32)
        dtemp = jnp.zeros((1, 128), F32)
        for h in range(GH):
            hr = slice(HD * h, HD * (h + 1))
            a, cosine, den = a_v[0, hr, :], a_v[1, hr, :], a_v[2, hr, :]
            da = head_block(dbase, h)
            ds = a * (da - jnp.sum(a * da, axis=1, keepdims=True))
            dt = jnp.sum(jnp.sum(ds * cosine, axis=1, keepdims=True), axis=0, keepdims=True)
            dtemp = jnp.where(lane48[:1] == g * GH + h, dt, dtemp)
            dcos = temp_ref[g * GH + h] * ds
            w = dcos * cosine
            row_v[hr, :] = -jnp.sum(w, axis=1, keepdims=True) / row_v[hr, :]
            dsk = dsk - place(jnp.broadcast_to(jnp.sum(w, axis=0, keepdims=True), (8, 128)), h)
            bd_v[1, hr, :] = place(dcos / den, h).astype(BF16)
        dsq_v[8:16, :] = dsk / skrow
        dsq_v[0:8, :] = jnp.concatenate(
            [row_v[128 * c:128 * (c + 1), :].T[:8] for c in range(3)], axis=1)
        if g == 0:
            dtemp_out[0:1, :] = dtemp
        else:
            dtemp_out[0:1, :] += dtemp

    def heads_v(g):
        def body(b):
            rows = block(b)
            cols = slice(g * GW, (g + 1) * GW)
            vc = slice((3 * g + 2) * GW, (3 * g + 3) * GW)
            a = bd_v[0]
            o = dot(qkv_v[rows, vc], a, 1, 1).astype(BF16)
            qkv_v[rows, vc] = dot(do_v[rows, cols], a, 1, 0).astype(BF16)
            do_v[rows, cols] = o
            ot_v[cols, rows] = o.T
        loop(body)

    def heads_qk(g):
        def body(b):
            rows = block(b)
            qc = slice(3 * g * GW, (3 * g + 1) * GW)
            kc = slice((3 * g + 1) * GW, (3 * g + 2) * GW)
            d = bd_v[1]
            q = qkv_v[rows, qc]
            k = qkv_v[rows, kc]
            dq = (dot(k, d, 1, 1) + q.astype(F32) * dsq_v[0:1, :]).astype(BF16)
            dk = (dot(q, d, 1, 0) + k.astype(F32) * dsq_v[8:9, :]).astype(BF16)
            qkv_v[rows, qc] = dq
            qkv_v[rows, kc] = dk
        loop(body)

    PART = {0: 2, 1: 0, 2: 1, 3: 5, 6: 3, 7: 4}

    def gw_chunks(ch, n):
        def half(m, carry):
            mr = pl.ds(pl.multiple_of(m * GW, GW), GW)
            if ch in PART:
                c0 = PART[ch] * GW
                res = dot(ut_v[mr, :], qkv_v[:, c0:c0 + n * GW], 1, 0)
            else:
                res = dot(ot_v[mr, :], dy_v[...], 1, 0)
            for i in range(n):
                gw_v[ch + i, pl.ds(2 * m, 2)] = res[:, i * GW:(i + 1) * GW].reshape(2, 2, SHARD, GW)
            return carry
        lax.fori_loop(0, 2, half, 0)

    def s1(ch):
        c = remote(gw_v.at[ch, :, 1 - core], r1.at[ch], s1_send.at[ch], s1_recv.at[ch], partner)
        c.start()
        held['s1', ch] = c

    def s2(ch):
        held['s1', ch].wait()
        for n, b in ((0, 1 - cb), (1, cb)):
            i = chip(1 - ca, b)
            r1[ch, i] += gw_v[ch, i, core]
            c = remote(r1.at[ch, i], r2.at[ch, b], s2_send.at[ch, b], s2_recv.at[ch, b], first)
            c.start()
            held['s2', ch, n] = c
        for b in (1 - cb, cb):
            i = chip(ca, b)
            r1[ch, i] += gw_v[ch, i, core]

    def s3(ch):
        held['s2', ch, 0].wait()
        r2[ch, 1 - cb] += r1[ch, chip(ca, 1 - cb)]
        c = remote(r2.at[ch, 1 - cb], r3.at[ch], s3_send.at[ch], s3_recv.at[ch], second)
        c.start()
        held['s3', ch] = c

    def s4(ch):
        held['s2', ch, 1].wait()
        held['s3', ch].wait()
        total = r3[ch] + (r2[ch, cb] + r1[ch, chip(ca, cb)])
        if ch in PART:
            g, p = divmod(PART[ch], 3)
            c0 = p * WIDTH + g * GW
            gwq_out[:, c0:c0 + GW] = total
        else:
            gwo_out[:, (ch - 4) * GW:(ch - 3) * GW] = total

    def final_dots(b):
        rows = slice(b * BLK, (b + 1) * BLK)
        du_v[b % 2] = dot(qkv_v[rows, :], w_v[...], 1, 1)
        do_v[rows, :] = (x_v[rows, :].astype(F32) + dot(do_v[rows, :], wo_v[...], 1, 0)).astype(BF16)

    def final_norm(b):
        dgain = jnp.zeros((8, WIDTH), F32)
        dbias = jnp.zeros((8, WIDTH), F32)
        for i in range(BLK // LNR):
            r0 = b * BLK + i * LNR
            sub = slice(r0, r0 + LNR)
            xhat, rstd = normed_rows(r0)
            du = du_v[b % 2, i * LNR:(i + 1) * LNR, :]
            dgain = dgain + jnp.sum((du * xhat).reshape(LNR // 8, 8, WIDTH), axis=0)
            dbias = dbias + jnp.sum(du.reshape(LNR // 8, 8, WIDTH), axis=0)
            dxh = du * gain
            m1 = jnp.mean(dxh, axis=-1, keepdims=True)
            m2 = jnp.mean(dxh * xhat, axis=-1, keepdims=True)
            dx = rstd * (dxh - m1 - xhat * m2)
            x_v[sub, :] = (dy_v[sub, :].astype(F32) + dx).astype(BF16)
        gb_v[0] += dgain
        gb_v[1] += dbias

    def gb_start(k):
        to = (partner, first, second)[k]
        c = remote(gbs_v.at[k], gbr_v.at[k], gb_send.at[k], gb_recv.at[k], to)
        c.start()
        held['gb', k] = c

    def gb_next(k):
        held['gb', k].wait()
        total = gbs_v[k] + gbr_v[k]
        if k < 2:
            gbs_v[k + 1] = total
            gb_start(k + 1)
        else:
            gb_out[...] = total

    sq_v[...] = jnp.zeros_like(sq_v)
    gb_v[...] = jnp.zeros_like(gb_v)
    dtemp_out[...] = jnp.zeros_like(dtemp_out)
    x_copy(0).wait()
    norm_block(0)
    w_copy(0, 0).wait()
    w_copy(0, 1).wait()
    for b in range(NBLK):
        if b + 1 < NBLK:
            x_copy(b + 1).wait()
            norm_block(b + 1)
        project(0, 0, 2, slice(b * BLK, (b + 1) * BLK))
    gram(0, MSG0[0])
    pl.semaphore_wait(barrier, 3)
    ar(0, 0)
    w_copy(0, 2).wait()
    wo_copy.wait()
    for b in range(NBLK):
        dy_copy(b).wait()
    loop(values_and_do)
    ar(0, 1)
    dgram(0, MSG0[1])
    ar(1, 0)
    for p in range(3):
        w_copy(1, p).wait()

    def project_1(b):
        project(1, 0, 3, block(b))
    lax.fori_loop(0, 2, lambda b, c: (project_1(b), c)[1], 0)
    ar(0, 2)
    ar(1, 1)
    lax.fori_loop(2, 4, lambda b, c: (project_1(b), c)[1], 0)
    gram(1, MSG0[2])
    ar(0, 3)
    ar(1, 2)
    dgram(1, MSG0[2] + PAIR + 16)
    ar(2, 0)
    ar(0, 4)
    attn(0, MSG0[0])
    ar(1, 3)
    ar(2, 1)
    heads_v(0)
    gw_chunks(0, 1)
    s1(0)
    ar(2, 2)
    ar(1, 4)
    attn_vjp(0, MSG0[0], MSG0[1])
    s2(0)
    heads_qk(0)
    ar(2, 3)
    gw_chunks(1, 2)
    s1(1)
    s1(2)
    ar(2, 4)
    attn(1, MSG0[2])
    s2(1)
    s2(2)
    s3(0)
    heads_v(1)
    gw_chunks(3, 1)
    s1(3)
    attn_vjp(1, MSG0[2], MSG0[2] + PAIR + 16)
    s2(3)
    s3(1)
    gw_chunks(4, 2)
    s1(4)
    s1(5)
    heads_qk(1)
    s2(4)
    s2(5)
    s3(2)
    gw_chunks(6, 2)
    s1(6)
    s1(7)
    final_dots(0)
    s2(6)
    s2(7)
    s3(3)
    final_norm(0)
    final_dots(1)
    s3(4)
    final_norm(1)
    final_dots(2)
    s3(5)
    final_norm(2)
    final_dots(3)
    s3(6)
    final_norm(3)
    gbs_v[0] = jnp.concatenate([jnp.sum(gb_v[i], axis=0, keepdims=True) for i in range(2)]
                               + [jnp.zeros((6, WIDTH), F32)], axis=0)
    gb_start(0)
    for ch in range(0, 4):
        s4(ch)
    gb_next(0)
    for ch in range(4, 6):
        s4(ch)
    gb_next(1)
    s3(7)
    s4(6)
    gb_next(2)
    s4(7)


def writer(out_v, gtok_v, gwq_v, gwo_v, gb_v, dtemp_v,
           out_hbm, gtok_hbm, gwq_hbm, gwo_hbm, gain_hbm, bias_hbm, dtemp_out, sem):
    pairs = [(gtok_v, gtok_hbm), (out_v, out_hbm), (gwq_v, gwq_hbm), (gwo_v, gwo_hbm),
             (gb_v.at[0], gain_hbm), (gb_v.at[1], bias_hbm)]
    copies = [pltpu.make_async_copy(src, dst, sem.at[i]) for i, (src, dst) in enumerate(pairs)]
    for c in copies:
        c.start()
    dtemp_out[...] = dtemp_v[0, :HEADS]
    for c in copies:
        c.wait()


def block_step(x, dy, ln_gain, ln_bias, w_qkv, w_out, temperature):
    hbm = pl.BlockSpec(memory_space=pl.ANY)
    vmem = pl.BlockSpec(memory_space=pltpu.VMEM)
    smem = pl.BlockSpec(memory_space=pltpu.SMEM)
    dma = pltpu.SemaphoreType.DMA
    gtok, out, gwq, gwo, gb, dtemp = pl.pallas_call(
        kernel,
        out_shape=(
            pltpu.VMEM((ROWS, WIDTH), BF16),
            pltpu.VMEM((ROWS, WIDTH), BF16),
            pltpu.VMEM((SHARD, TOT), F32),
            pltpu.VMEM((SHARD, WIDTH), F32),
            pltpu.VMEM((8, WIDTH), F32),
            pltpu.VMEM((8, 128), F32),
        ),
        in_specs=[smem, vmem, vmem, hbm, hbm, hbm, hbm],
        out_specs=(vmem,) * 6,
        scratch_shapes=[
            pltpu.VMEM((ROWS, WIDTH), BF16),
            pltpu.VMEM((ROWS, WIDTH), BF16),
            pltpu.VMEM((WIDTH, ROWS), BF16),
            pltpu.VMEM((ROWS, TOT), BF16),
            pltpu.VMEM((WIDTH, ROWS), BF16),
            pltpu.VMEM((WIDTH, TOT), BF16),
            pltpu.VMEM((WIDTH, WIDTH), BF16),
            pltpu.VMEM((GW, GW), F32),
            pltpu.VMEM((2, 2, 8, GW), F32),
            pltpu.VMEM((3, GW, 128), F32),
            pltpu.VMEM((2, GW, GW), BF16),
            pltpu.VMEM((16, GW), F32),
            pltpu.VMEM((GW, 128), F32),
            pltpu.VMEM((800, 128), F32),
            pltpu.VMEM((400, 128), F32),
            pltpu.VMEM((400, 128), F32),
            pltpu.VMEM((400, 128), F32),
            pltpu.VMEM((800, 128), F32),
            pltpu.VMEM((CHUNKS, 4, 2, SHARD, GW), F32),
            pltpu.VMEM((CHUNKS, 4, SHARD, GW), F32),
            pltpu.VMEM((CHUNKS, 2, SHARD, GW), F32),
            pltpu.VMEM((CHUNKS, SHARD, GW), F32),
            pltpu.VMEM((2, BLK, WIDTH), F32),
            pltpu.VMEM((2, 8, WIDTH), F32),
            pltpu.VMEM((3, 8, WIDTH), F32),
            pltpu.VMEM((3, 8, WIDTH), F32),
            dma((2, NBLK)), dma((7,)),
            dma((3, 4)), dma((3, 4)),
            dma((CHUNKS,)), dma((CHUNKS,)),
            dma((CHUNKS, 2)), dma((CHUNKS, 2)),
            dma((CHUNKS,)), dma((CHUNKS,)),
            dma((3,)), dma((3,)),
        ],
        compiler_params=pltpu.CompilerParams(
            collective_id=0, has_side_effects=True, vmem_limit_bytes=58000000),
    )(temperature, ln_gain, ln_bias, x, dy, w_qkv, w_out)
    return pl.pallas_call(
        writer,
        out_shape=(
            jax.ShapeDtypeStruct((ROWS, WIDTH), BF16),
            jax.ShapeDtypeStruct((ROWS, WIDTH), BF16),
            jax.ShapeDtypeStruct((SHARD, TOT), F32),
            jax.ShapeDtypeStruct((SHARD, WIDTH), F32),
            jax.ShapeDtypeStruct((WIDTH,), F32),
            jax.ShapeDtypeStruct((WIDTH,), F32),
            jax.ShapeDtypeStruct((HEADS,), F32),
        ),
        in_specs=[vmem] * 6,
        out_specs=(hbm,) * 6 + (vmem,),
        scratch_shapes=[dma((6,))],
        compiler_params=pltpu.CompilerParams(vmem_limit_bytes=1000000),
    )(out, gtok, gwq, gwo, gb, dtemp)


def solution(mesh):
    row_spec = P(('dp', 'sp'), None)
    part_spec = P('dp')
    full_spec = P()

    return jax.shard_map(block_step, mesh=mesh,
                         in_specs=(row_spec, row_spec, full_spec, full_spec, full_spec, full_spec, full_spec),
                         out_specs=(row_spec, row_spec, row_spec, row_spec, part_spec, part_spec, part_spec),
                         check_vma=False)
```

```python
import jax
import jax.numpy as jnp
from jax import lax
from jax.experimental import pallas as pl
from jax.experimental.pallas import tpu as pltpu
from jax.sharding import PartitionSpec as P

F32 = jnp.float32
BF16 = jnp.bfloat16
MESH = pl.DeviceIdType.MESH

ROWS = 2048
WIDTH = 768
HEADS = 16
HD = 48
GW = 384
GH = 8
BLK = 512
NBLK = ROWS // BLK
BIG = 1024
FINE = 256
NFINE = ROWS // FINE
LNR = 32
PAIR = 192
TOT = 2304
LANES = 128
TILE = 256
SPLIT = 5
MSG = (208, 208, 192, 192)
MSG0 = (0, 208, 416, 608)
PAY = 800
SLOTS = 4
ORDER = ((0, 1, 2), (4, 5, 3))
SHARD = 96
CHUNKS = 8


def dot(a, b, ca, cb):
    return lax.dot_general(a, b, (((ca,), (cb,)), ((), ())), preferred_element_type=F32)


def kernel(temp_ref, gain_ref, bias_ref, x_hbm, dy_hbm, wqkv_hbm, wout_hbm,
           x_v, do_v, gwq_out, gwo_out, gb_out, dtemp_out,
           dy_v, u_v, ut_v, qkv_v, v_v, ot_v, w_v, wo_v,
           gm_v, sq_v, a_v, bd_v, dsq_v, row_v, pay_v, ar1, ar2, ar3, sum_v,
           gw_v, r1, r2, r3, du0, du1, gb_v, gbs_v, gbr_v,
           in_sem, w_sem, x_sem,
           ar_send, ar_recv, s1_send, s1_recv, s2_send, s2_recv, s3_send, s3_recv, gb_send, gb_recv):
    dp = lax.axis_index('dp')
    me = lax.axis_index('sp')
    core = me % 2
    cx = (me // 2) % 2
    cy = me // 4
    partner = me + 1 - 2 * core
    xn = me + 2 - 4 * cx
    yn = me + 4 - 8 * cy
    first = xn + core * (yn - xn)
    second = yn + core * (xn - yn)
    diagonal = xn + 4 - 8 * cy
    ca = cx + core * (cy - cx)
    cb = cy + core * (cx - cy)

    def chip(a, b):
        return a * (1 + core) + b * (2 - core)

    def dev(i):
        return (dp, i)

    def remote(src, dst, ss, rs, to):
        return pltpu.make_async_remote_copy(src_ref=src, dst_ref=dst, send_sem=ss, recv_sem=rs,
                                            device_id=dev(to), device_id_type=MESH)

    barrier = pltpu.get_barrier_semaphore()
    for peer in (partner, xn, yn, diagonal):
        pl.semaphore_signal(barrier, inc=1, device_id=dev(peer), device_id_type=MESH)

    def cols(g, p):
        return slice(ORDER[g][p] * GW, (ORDER[g][p] + 1) * GW)

    def w_copy(g, p):
        return pltpu.make_async_copy(wqkv_hbm.at[:, pl.ds(p * WIDTH + g * GW, GW)],
                                     w_v.at[:, pl.ds(ORDER[g][p] * GW, GW)], w_sem.at[ORDER[g][p]])

    wo_copy = pltpu.make_async_copy(wout_hbm, wo_v, w_sem.at[6])

    def x_copy(b):
        rows = pl.ds(b * FINE, FINE)
        return pltpu.make_async_copy(x_hbm.at[rows], x_v.at[rows], x_sem.at[b])

    def dy_copy(b):
        rows = pl.ds(b * BLK, BLK)
        return pltpu.make_async_copy(dy_hbm.at[rows], dy_v.at[rows], in_sem.at[b])

    for b in range(2):
        x_copy(b).start()
    for p in range(2):
        w_copy(0, p).start()
    for b in range(2, NFINE):
        x_copy(b).start()
    for p in range(2):
        w_copy(1, p).start()
    for g in range(2):
        w_copy(g, 2).start()
    wo_copy.start()
    for b in range(NBLK):
        dy_copy(b).start()

    gain = gain_ref[...].reshape(1, WIDTH)
    bias = bias_ref[...].reshape(1, WIDTH)

    def loop(f, hooks=(), lo=0, hi=NBLK):
        def body(b, carry):
            f(b)
            for at, hook in hooks:
                pl.when(b == at)(hook)
            return carry
        lax.fori_loop(lo, hi, body, 0)

    def block(b, n=BLK):
        return pl.ds(pl.multiple_of(b * n, n), n)

    def normed_rows(r0):
        xf = x_v[pl.ds(r0, LNR), :].astype(F32)
        c = xf - jnp.mean(xf, axis=-1, keepdims=True)
        rstd = lax.rsqrt(jnp.mean(c * c, axis=-1, keepdims=True) + 1e-6)
        return c * rstd, rstd

    def norm_block(b):
        for r0 in range(b * BLK, (b + 1) * BLK, LNR):
            if b == 0 and r0 % FINE == 0:
                x_copy(r0 // FINE).wait()
            xhat, _ = normed_rows(r0)
            u_v[r0:r0 + LNR, :] = (xhat * gain + bias).astype(BF16)

    def sumsq(v):
        vf = v.astype(F32)
        return jnp.sum((vf * vf).reshape(-1, 8, GW), axis=0)

    def project(n, rows):
        c = slice(n * WIDTH, (n + 1) * WIDTH)
        res = dot(u_v[rows, :], w_v[:, c], 1, 0).astype(BF16)
        if n == 1:
            v_v[rows, :] = res
        else:
            qkv_v[rows, c] = res
            sq_v[n // 2, 0] += sumsq(res[:, :GW])
            sq_v[n // 2, 1] += sumsq(res[:, GW:])

    def values_and_do(b):
        rows = block(b)
        project(1, rows)
        do_v[rows, :] = dot(dy_v[rows, :], wo_v[...], 1, 1).astype(BF16)
        ut_v[:, rows] = u_v[rows, :].T

    lane48 = lax.broadcasted_iota(jnp.int32, (HD, LANES), 1)
    ok = lane48 < HD

    def local(h):
        t = int(h >= SPLIT)
        return t, HD * h - LANES * t

    def pack(left, lc, right, rc, base):
        for t in range(2):
            off = LANES * t
            gm_v[t] = dot(left[:, lc + off:lc + off + TILE], right[:, rc + off:rc + off + TILE], 0, 0)

        def piece(h, to):
            t, r = local(h)
            lo = r // LANES * LANES
            n = LANES if r + HD <= lo + LANES else TILE
            v = gm_v[t, r:r + HD, lo:lo + n]
            move = (to - (r - lo)) % n
            if move:
                v = pltpu.roll(v, move, 1)
            return v[:, :LANES]
        for p in range(GH // 2):
            a = piece(2 * p, 0)
            d = piece(2 * p + 1, LANES // 2)
            side = lane48 - LANES // 2
            both = jnp.where(ok, a, jnp.where((side >= 0) & (side < HD), d, 0.0))
            pay_v[base + HD * p:base + HD * (p + 1), :] = both

    def gram(g):
        pack(qkv_v, cols(g, 0).start, qkv_v, cols(g, 1).start, MSG0[g])
        r0 = MSG0[g] + PAIR
        pay_v[r0:r0 + 16, :] = jnp.zeros((16, LANES), F32)
        for p in range(2):
            row = jnp.sum(sq_v[g, p], axis=0, keepdims=True)
            for c in range(3):
                pay_v[r0 + 3 * p + c:r0 + 3 * p + c + 1, :] = row[:, LANES * c:LANES * (c + 1)]

    def dgram(g):
        pack(do_v, g * GW, v_v, g * GW, MSG0[2 + g])

    held = {}

    def ar(m, k):
        half = MSG[m] // 2
        mine = pl.ds(pl.multiple_of(MSG0[m] + core * half, 8), half)
        theirs = pl.ds(pl.multiple_of(MSG0[m] + (1 - core) * half, 8), half)
        slot = pl.ds(MSG0[m] // 2, half)
        steps = ((pay_v.at[theirs], ar1.at[slot], partner), (pay_v.at[mine], ar2.at[slot], first),
                 (pay_v.at[mine], ar3.at[slot], second), (sum_v.at[mine], sum_v.at[mine], partner))

        def copy(n):
            src, dst, to = steps[n]
            return remote(src, dst, ar_send.at[m, n], ar_recv.at[m, n], to)
        if k:
            copy(k - 1).wait()
        if k == 1:
            pay_v[mine, :] = ar1[slot, :] + pay_v[mine, :]
        elif k == 2:
            pay_v[mine, :] = ar2[slot, :] + pay_v[mine, :]
        elif k == 3:
            sum_v[mine, :] = ar3[slot, :] + pay_v[mine, :]
        if k < 4:
            copy(k).start()

    def hook(*steps):
        def run():
            for m, k in steps:
                ar(m, k)
        return run

    def place(v, at, n):
        wide = jnp.concatenate([v, jnp.zeros((v.shape[0], n - LANES), v.dtype)], axis=1)
        return pltpu.roll(wide, at, 1) if at else wide

    def put(g, k, h, v):
        t, r = local(h)
        bd_v[g, k, t, r:r + HD, :] = place(v, r, TILE).astype(BF16)

    def head_block(base, h):
        r0 = base + HD * (h // 2)
        both = sum_v[r0:r0 + HD, :]
        if h % 2:
            both = pltpu.roll(both, LANES // 2, 1)
        return jnp.where(ok, both, 0.0)

    def sums(g, p):
        r0 = MSG0[g] + PAIR + 3 * p
        return jnp.concatenate([sum_v[r0 + c:r0 + c + 1, :] for c in range(3)], axis=1)

    def attn(g):
        sqrow = sums(g, 0)
        skwide = jnp.broadcast_to(sums(g, 1), (8, GW))
        for c in range(3):
            lanes = slice(LANES * c, LANES * (c + 1))
            row_v[g, lanes, :] = jnp.broadcast_to(sqrow[:, lanes], (LANES, LANES)).T
        for h in range(GH):
            hr = slice(HD * h, HD * (h + 1))
            skh = pltpu.roll(skwide, GW - HD * h, 1) if h else skwide
            skh = jnp.where(ok, jnp.broadcast_to(skh[:1, :LANES], (HD, LANES)), 1.0)
            den = jnp.sqrt(row_v[g, hr, :]) * jnp.sqrt(skh)
            cosine = head_block(MSG0[g], h) / den
            logit = jnp.where(ok, temp_ref[g * GH + h] * cosine, -jnp.inf)
            e = jnp.where(ok, jnp.exp(logit - jnp.max(logit, axis=1, keepdims=True)), 0.0)
            a = e / jnp.sum(e, axis=1, keepdims=True)
            for i, v in enumerate((a, cosine, den)):
                a_v[g, i, hr, :] = v
            put(g, 0, h, a)

    def attn_vjp(g):
        dsk = jnp.zeros((8, GW), F32)
        dtemp = jnp.zeros((1, LANES), F32)
        for h in range(GH):
            hr = slice(HD * h, HD * (h + 1))
            a, cosine, den = [a_v[g, i, hr, :] for i in range(3)]
            da = head_block(MSG0[2 + g], h)
            ds = a * (da - jnp.sum(a * da, axis=1, keepdims=True))
            dt = jnp.sum(jnp.sum(ds * cosine, axis=1, keepdims=True), axis=0, keepdims=True)
            dtemp = jnp.where(lane48[:1] == g * GH + h, dt, dtemp)
            dcos = temp_ref[g * GH + h] * ds
            w = dcos * cosine
            row_v[g, hr, :] = -jnp.sum(w, axis=1, keepdims=True) / row_v[g, hr, :]
            dsk = dsk - place(jnp.broadcast_to(jnp.sum(w, axis=0, keepdims=True), (8, LANES)), HD * h, GW)
            put(g, 1, h, dcos / den)
        dsq_v[g, 1] = dsk / sums(g, 1)
        dsq_v[g, 0] = jnp.concatenate([row_v[g, LANES * c:LANES * (c + 1), :].T[:8] for c in range(3)], axis=1)
        dtemp_out[:1, :] += dtemp

    def head_dot(g, x, k, c):
        lo = dot(x[:, :TILE], bd_v[g, k, 0], 1, c)
        hi = dot(x[:, LANES:], bd_v[g, k, 1], 1, c)
        return jnp.concatenate([lo[:, :LANES], lo[:, LANES:] + hi[:, :LANES], hi[:, LANES:]], axis=1)

    def heads_v(g):
        def body(b):
            rows = block(b, BIG)
            oc = slice(g * GW, (g + 1) * GW)
            qkv_v[rows, cols(g, 2)] = head_dot(g, do_v[rows, oc], 0, 0).astype(BF16)
            o = head_dot(g, v_v[rows, oc], 0, 1).astype(BF16)
            u_v[rows, oc] = o
            ot_v[oc, rows] = o.T
        loop(body, hi=ROWS // BIG)

    def heads_qk(g):
        def body(b):
            rows = block(b, BIG)
            q = qkv_v[rows, cols(g, 0)]
            k = qkv_v[rows, cols(g, 1)]
            dq = head_dot(g, k, 1, 1) + q.astype(F32) * dsq_v[g, 0, :1, :]
            dk = head_dot(g, q, 1, 0) + k.astype(F32) * dsq_v[g, 1, :1, :]
            qkv_v[rows, cols(g, 0)] = dq.astype(BF16)
            qkv_v[rows, cols(g, 1)] = dk.astype(BF16)
        loop(body, hi=ROWS // BIG)

    PART = ((0, 2), (1, 2), None, None, (0, 0), (0, 1), (1, 0), (1, 1))

    def s1(k, m):
        two = pl.ds(2 * m, 2)
        return remote(gw_v.at[k % SLOTS, two, 1 - core], r1.at[k, two], s1_send.at[k, m], s1_recv.at[k, m], partner)

    def gw_chunks(ch, n):
        def half(m, carry):
            mr = pl.ds(pl.multiple_of(m * GW, GW), GW)
            if PART[ch]:
                c0 = cols(*PART[ch]).start
                res = dot(ut_v[mr, :], qkv_v[:, c0:c0 + n * GW], 1, 0)
            else:
                res = dot(ot_v[mr, :], dy_v[...], 1, 0)
            for i in range(n):
                gw_v[(ch + i) % SLOTS, pl.ds(2 * m, 2)] = res[:, i * GW:(i + 1) * GW].reshape(2, 2, SHARD, GW)
            for i in range(n):
                s1(ch + i, m).start()
            return carry
        lax.fori_loop(0, 2, half, 0)

    def s2_copy(ch, b):
        return remote(r1.at[ch, chip(1 - ca, b)], r2.at[ch, b], s2_send.at[ch, b], s2_recv.at[ch, b], first)

    def s2_near(ch, b):
        i = chip(ca, b)
        r1[ch, i] += gw_v[ch % SLOTS, i, core]

    def s2_far(ch, b):
        i = chip(1 - ca, b)
        r1[ch, i] += gw_v[ch % SLOTS, i, core]
        s2_copy(ch, b).start()

    def s2(ch, last=False):
        for m in range(2):
            s1(ch, m).wait()
        s2_far(ch, 1 - cb)
        if not last:
            s2_far(ch, cb)
        s2_near(ch, 1 - cb)
        s2_near(ch, cb)

    def s3_copy(ch):
        return remote(r2.at[ch, 1 - cb], r3.at[ch], s3_send.at[ch], s3_recv.at[ch], second)

    def s3(ch):
        s2_copy(ch, 1 - cb).wait()
        r2[ch, 1 - cb] += r1[ch, chip(ca, 1 - cb)]
        s3_copy(ch).start()

    def s4(ch):
        s2_copy(ch, cb).wait()
        s3_copy(ch).wait()
        total = r3[ch] + (r2[ch, cb] + r1[ch, chip(ca, cb)])
        if PART[ch]:
            g, p = PART[ch]
            c0 = p * WIDTH + g * GW
            gwq_out[:, c0:c0 + GW] = total
        else:
            gwo_out[:, (ch - 2) * GW:(ch - 1) * GW] = total

    def out_tokens(b):
        rows = block(b)
        do_v[rows, :] = (x_v[rows, :].astype(F32) + dot(u_v[rows, :], wo_v[...], 1, 0)).astype(BF16)

    def final_dots(b):
        (du0, du1)[b % 2][...] = dot(qkv_v[b * BLK:(b + 1) * BLK, :], w_v[...], 1, 1)

    def final_norm(b):
        du_ref = (du0, du1)[b % 2]
        dgain = jnp.zeros((8, WIDTH), F32)
        dbias = jnp.zeros((8, WIDTH), F32)
        for i in range(0, BLK, LNR):
            sub = slice(b * BLK + i, b * BLK + i + LNR)
            xhat, rstd = normed_rows(b * BLK + i)
            du = du_ref[i:i + LNR, :]
            dgain = dgain + jnp.sum((du * xhat).reshape(-1, 8, WIDTH), axis=0)
            dbias = dbias + jnp.sum(du.reshape(-1, 8, WIDTH), axis=0)
            dxh = du * gain
            m1 = jnp.mean(dxh, axis=-1, keepdims=True)
            m2 = jnp.mean(dxh * xhat, axis=-1, keepdims=True)
            dx = rstd * (dxh - m1 - xhat * m2)
            x_v[sub, :] = (dy_v[sub, :].astype(F32) + dx).astype(BF16)
        gb_v[0] += dgain
        gb_v[1] += dbias

    def last_step(b):
        if b < NBLK:
            final_dots(b)
        if b:
            final_norm(b - 1)

    def gb_start():
        both = [jnp.sum(gb_v[i], axis=0, keepdims=True) for i in range(2)]
        gbs_v[0] = jnp.concatenate(both + [jnp.zeros((6, WIDTH), F32)], axis=0)
        c = remote(gbs_v.at[0], gbs_v.at[1], gb_send.at[3], gb_recv.at[3], partner)
        c.start()
        held['gb', 3] = c

    def gb_chips():
        held['gb', 3].wait()
        here = me // 2
        gbr_v[here] = gbs_v[0] + gbs_v[1]
        for k, to in enumerate((first, second, diagonal)):
            c = remote(gbr_v.at[here], gbr_v.at[here], gb_send.at[k], gb_recv.at[k], to)
            c.start()
            held['gb', k] = c

    def gb_end():
        for k in range(3):
            held['gb', k].wait()
        gb_out[...] = (gbr_v[0] + gbr_v[1]) + (gbr_v[2] + gbr_v[3])

    for ref in (sq_v, gb_v, dtemp_out, bd_v):
        ref[...] = jnp.zeros_like(ref)
    def first_step(b):
        if b + 1 < NBLK:
            for i in range(2):
                x_copy(2 * (b + 1) + i).wait()
            norm_block(b + 1)
        project(0, slice(b * BLK, (b + 1) * BLK))

    norm_block(0)
    for p in range(2):
        w_copy(0, p).wait()
    for b in range(NBLK):
        first_step(b)
    gram(0)
    pl.semaphore_wait(barrier, 4)
    ar(0, 0)
    for p in range(2):
        w_copy(1, p).wait()
    loop(lambda b: project(2, block(b)), ((1, hook((0, 1))),))
    gram(1)
    ar(1, 0)
    for g in range(2):
        w_copy(g, 2).wait()
    wo_copy.wait()
    for b in range(NBLK):
        dy_copy(b).wait()
    loop(values_and_do, ((0, hook((0, 2), (1, 1))), (2, hook((0, 3))), (3, hook((1, 2), (0, 4)))))
    attn(0)
    heads_v(0)
    ar(1, 3)
    gw_chunks(0, 1)
    dgram(0)
    ar(2, 0)
    ar(1, 4)
    attn(1)
    ar(2, 1)
    s2(0)
    heads_v(1)
    gw_chunks(1, 1)
    ar(2, 2)
    dgram(1)
    ar(3, 0)
    s2(1)
    ar(3, 1)
    s3(0)
    gw_chunks(2, 2)
    ar(2, 3)

    def mid():
        s2(2)
        s2(3)

    def late():
        ar(2, 4)
        s3(1)

    loop(out_tokens, ((0, mid), (1, late)), hi=NBLK - 1)
    attn_vjp(0)
    heads_qk(0)
    ar(3, 2)
    gw_chunks(4, 2)
    out_tokens(NBLK - 1)
    ar(3, 3)
    s2(4)
    s2(5)
    s3(2)
    ar(3, 4)
    attn_vjp(1)
    heads_qk(1)
    gw_chunks(6, 2)
    s3(3)
    last_step(0)
    s2(6)
    s2(7, True)
    s3(4)
    for b in range(1, NBLK + 1):
        last_step(b)
        if b in (2, 3):
            s3(3 + b)
    gb_start()
    for ch in range(4):
        s4(ch)
    gb_chips()
    s2_far(7, cb)
    s4(4)
    s3(7)
    s4(5)
    s4(6)
    gb_end()
    s4(7)


def writer(out_v, gtok_v, gwq_v, gwo_v, gb_v, dtemp_v,
           out_hbm, gtok_hbm, gwq_hbm, gwo_hbm, gain_hbm, bias_hbm, dtemp_out, sem):
    pairs = [(gtok_v, gtok_hbm), (out_v, out_hbm), (gwq_v, gwq_hbm), (gwo_v, gwo_hbm),
             (gb_v.at[0], gain_hbm), (gb_v.at[1], bias_hbm)]
    copies = [pltpu.make_async_copy(src, dst, sem.at[i]) for i, (src, dst) in enumerate(pairs)]
    for c in copies:
        c.start()
    dtemp_out[...] = dtemp_v[0, :HEADS]
    for c in copies:
        c.wait()


def block_step(x, dy, ln_gain, ln_bias, w_qkv, w_out, temperature):
    hbm = pl.BlockSpec(memory_space=pl.ANY)
    vmem = pl.BlockSpec(memory_space=pltpu.VMEM)
    smem = pl.BlockSpec(memory_space=pltpu.SMEM)
    dma = pltpu.SemaphoreType.DMA
    gtok, out, gwq, gwo, gb, dtemp = pl.pallas_call(
        kernel,
        out_shape=(
            pltpu.VMEM((ROWS, WIDTH), BF16),
            pltpu.VMEM((ROWS, WIDTH), BF16),
            pltpu.VMEM((SHARD, TOT), F32),
            pltpu.VMEM((SHARD, WIDTH), F32),
            pltpu.VMEM((8, WIDTH), F32),
            pltpu.VMEM((8, 128), F32),
        ),
        in_specs=[smem, vmem, vmem, hbm, hbm, hbm, hbm],
        out_specs=(vmem,) * 6,
        scratch_shapes=[
            pltpu.VMEM((ROWS, WIDTH), BF16),
            pltpu.VMEM((ROWS, WIDTH), BF16),
            pltpu.VMEM((WIDTH, ROWS), BF16),
            pltpu.VMEM((ROWS, TOT), BF16),
            pltpu.VMEM((ROWS, WIDTH), BF16),
            pltpu.VMEM((WIDTH, ROWS), BF16),
            pltpu.VMEM((WIDTH, TOT), BF16),
            pltpu.VMEM((WIDTH, WIDTH), BF16),
            pltpu.VMEM((2, TILE, TILE), F32),
            pltpu.VMEM((2, 2, 8, GW), F32),
            pltpu.VMEM((2, 3, GW, LANES), F32),
            pltpu.VMEM((2, 2, 2, TILE, TILE), BF16),
            pltpu.VMEM((2, 2, 8, GW), F32),
            pltpu.VMEM((2, GW, LANES), F32),
            pltpu.VMEM((PAY, LANES), F32),
            pltpu.VMEM((PAY // 2, LANES), F32),
            pltpu.VMEM((PAY // 2, LANES), F32),
            pltpu.VMEM((PAY // 2, LANES), F32),
            pltpu.VMEM((PAY, LANES), F32),
            pltpu.VMEM((SLOTS, 4, 2, SHARD, GW), F32),
            pltpu.VMEM((CHUNKS, 4, SHARD, GW), F32),
            pltpu.VMEM((CHUNKS, 2, SHARD, GW), F32),
            pltpu.VMEM((CHUNKS, SHARD, GW), F32),
            pltpu.VMEM((BLK, WIDTH), F32),
            pltpu.VMEM((BLK, WIDTH), F32),
            pltpu.VMEM((2, 8, WIDTH), F32),
            pltpu.VMEM((2, 8, WIDTH), F32),
            pltpu.VMEM((4, 8, WIDTH), F32),
            dma((NBLK,)), dma((7,)), dma((NFINE,)),
            dma((4, 4)), dma((4, 4)),
            dma((CHUNKS, 2)), dma((CHUNKS, 2)),
            dma((CHUNKS, 2)), dma((CHUNKS, 2)),
            dma((CHUNKS,)), dma((CHUNKS,)),
            dma((4,)), dma((4,)),
        ],
        compiler_params=pltpu.CompilerParams(
            collective_id=0, has_side_effects=True, vmem_limit_bytes=59400000),
    )(temperature, ln_gain, ln_bias, x, dy, w_qkv, w_out)
    return pl.pallas_call(
        writer,
        out_shape=(
            jax.ShapeDtypeStruct((ROWS, WIDTH), BF16),
            jax.ShapeDtypeStruct((ROWS, WIDTH), BF16),
            jax.ShapeDtypeStruct((SHARD, TOT), F32),
            jax.ShapeDtypeStruct((SHARD, WIDTH), F32),
            jax.ShapeDtypeStruct((WIDTH,), F32),
            jax.ShapeDtypeStruct((WIDTH,), F32),
            jax.ShapeDtypeStruct((HEADS,), F32),
        ),
        in_specs=[vmem] * 6,
        out_specs=(hbm,) * 6 + (vmem,),
        scratch_shapes=[dma((6,))],
        compiler_params=pltpu.CompilerParams(vmem_limit_bytes=1000000),
    )(out, gtok, gwq, gwo, gb, dtemp)


def solution(mesh):
    row_spec = P(('dp', 'sp'), None)
    part_spec = P('dp')
    full_spec = P()

    return jax.shard_map(block_step, mesh=mesh,
                         in_specs=(row_spec, row_spec, full_spec, full_spec, full_spec, full_spec, full_spec),
                         out_specs=(row_spec, row_spec, row_spec, row_spec, part_spec, part_spec, part_spec),
                         check_vma=False)
```

```python
import jax
import jax.numpy as jnp
from jax import lax
from jax.experimental import pallas as pl
from jax.experimental.pallas import tpu as pltpu
from jax.sharding import PartitionSpec as P

F32 = jnp.float32
BF16 = jnp.bfloat16
MESH = pl.DeviceIdType.MESH

ROWS = 2048
WIDTH = 768
HEADS = 16
HD = 48
GW = 384
GH = 8
BLK = 512
NBLK = ROWS // BLK
BIG = 1024
FINE = 256
NFINE = ROWS // FINE
LNR = 32
PAIR = 192
TOT = 2304
LANES = 128
TILE = 256
SPLIT = 5
MSG = (208, 208, 192, 192)
MSG0 = (0, 208, 416, 608)
PAY = 800
SLOTS = 4
ORDER = ((0, 1, 2), (4, 5, 3))
SHARD = 96
CHUNKS = 8


def dot(a, b, ca, cb):
    return lax.dot_general(a, b, (((ca,), (cb,)), ((), ())), preferred_element_type=F32)


def kernel(temp_ref, gain_ref, bias_ref, x_hbm, dy_hbm, wqkv_hbm, wout_hbm,
           x_v, do_v, gwq_out, gwo_out, gb_out, dtemp_out,
           dy_v, u_v, ut_v, qkv_v, v_v, ot_v, w_v, wo_v,
           gm_v, sq_v, a_v, bd_v, dsq_v, row_v, pay_v, ar1, ar2, ar3, sum_v,
           gw_v, r1, r2, r3, du0, du1, gb_v, gbs_v, gbr_v,
           in_sem, w_sem, x_sem,
           ar_send, ar_recv, s1_send, s1_recv, s2_send, s2_recv, s3_send, s3_recv, gb_send, gb_recv):
    dp = lax.axis_index('dp')
    me = lax.axis_index('sp')
    core = me % 2
    cx = (me // 2) % 2
    cy = me // 4
    partner = me + 1 - 2 * core
    xn = me + 2 - 4 * cx
    yn = me + 4 - 8 * cy
    first = xn + core * (yn - xn)
    second = yn + core * (xn - yn)
    diagonal = xn + 4 - 8 * cy
    ca = cx + core * (cy - cx)
    cb = cy + core * (cx - cy)

    def chip(a, b):
        return a * (1 + core) + b * (2 - core)

    def dev(i):
        return (dp, i)

    def remote(src, dst, ss, rs, to):
        return pltpu.make_async_remote_copy(src_ref=src, dst_ref=dst, send_sem=ss, recv_sem=rs,
                                            device_id=dev(to), device_id_type=MESH)

    barrier = pltpu.get_barrier_semaphore()
    for peer in (partner, xn, yn, diagonal):
        pl.semaphore_signal(barrier, inc=1, device_id=dev(peer), device_id_type=MESH)

    def cols(g, p):
        return slice(ORDER[g][p] * GW, (ORDER[g][p] + 1) * GW)

    def w_copy(g, p):
        return pltpu.make_async_copy(wqkv_hbm.at[:, pl.ds(p * WIDTH + g * GW, GW)],
                                     w_v.at[:, pl.ds(ORDER[g][p] * GW, GW)], w_sem.at[ORDER[g][p]])

    wo_copy = pltpu.make_async_copy(wout_hbm, wo_v, w_sem.at[6])

    def x_copy(b):
        rows = pl.ds(b * FINE, FINE)
        return pltpu.make_async_copy(x_hbm.at[rows], x_v.at[rows], x_sem.at[b])

    def dy_copy(b):
        rows = pl.ds(b * BLK, BLK)
        return pltpu.make_async_copy(dy_hbm.at[rows], dy_v.at[rows], in_sem.at[b])

    for b in range(2):
        x_copy(b).start()
    for p in range(2):
        w_copy(0, p).start()
    for b in range(2, NFINE):
        x_copy(b).start()
    for p in range(2):
        w_copy(1, p).start()
    for g in range(2):
        w_copy(g, 2).start()
    wo_copy.start()
    for b in range(NBLK):
        dy_copy(b).start()

    gain = gain_ref[...].reshape(1, WIDTH)
    bias = bias_ref[...].reshape(1, WIDTH)

    def loop(f, hooks=(), lo=0, hi=NBLK):
        def body(b, carry):
            f(b)
            for at, hook in hooks:
                pl.when(b == at)(hook)
            return carry
        lax.fori_loop(lo, hi, body, 0)

    def block(b, n=BLK):
        return pl.ds(pl.multiple_of(b * n, n), n)

    def normed_rows(r0):
        xf = x_v[pl.ds(r0, LNR), :].astype(F32)
        c = xf - jnp.mean(xf, axis=-1, keepdims=True)
        rstd = lax.rsqrt(jnp.mean(c * c, axis=-1, keepdims=True) + 1e-6)
        return c * rstd, rstd

    def norm_block(b):
        for r0 in range(b * BLK, (b + 1) * BLK, LNR):
            if b == 0 and r0 % FINE == 0:
                x_copy(r0 // FINE).wait()
            xhat, _ = normed_rows(r0)
            u_v[r0:r0 + LNR, :] = (xhat * gain + bias).astype(BF16)

    def sumsq(v):
        vf = v.astype(F32)
        return jnp.sum((vf * vf).reshape(-1, 8, GW), axis=0)

    def project(n, rows):
        c = slice(n * WIDTH, (n + 1) * WIDTH)
        res = dot(u_v[rows, :], w_v[:, c], 1, 0).astype(BF16)
        if n == 1:
            v_v[rows, :] = res
        else:
            qkv_v[rows, c] = res
            sq_v[n // 2, 0] += sumsq(res[:, :GW])
            sq_v[n // 2, 1] += sumsq(res[:, GW:])

    def values_and_do(b):
        rows = block(b)
        project(1, rows)
        do_v[rows, :] = dot(dy_v[rows, :], wo_v[...], 1, 1).astype(BF16)
        ut_v[:, rows] = u_v[rows, :].T

    lane48 = lax.broadcasted_iota(jnp.int32, (HD, LANES), 1)
    ok = lane48 < HD

    def local(h):
        t = int(h >= SPLIT)
        return t, HD * h - LANES * t

    def pack(left, lc, right, rc, base):
        for t in range(2):
            off = LANES * t
            gm_v[t] = dot(left[:, lc + off:lc + off + TILE], right[:, rc + off:rc + off + TILE], 0, 0)

        def piece(h, to):
            t, r = local(h)
            lo = r // LANES * LANES
            n = LANES if r + HD <= lo + LANES else TILE
            v = gm_v[t, r:r + HD, lo:lo + n]
            move = (to - (r - lo)) % n
            if move:
                v = pltpu.roll(v, move, 1)
            return v[:, :LANES]
        for p in range(GH // 2):
            a = piece(2 * p, 0)
            d = piece(2 * p + 1, LANES // 2)
            side = lane48 - LANES // 2
            both = jnp.where(ok, a, jnp.where((side >= 0) & (side < HD), d, 0.0))
            pay_v[base + HD * p:base + HD * (p + 1), :] = both

    def gram(g):
        pack(qkv_v, cols(g, 0).start, qkv_v, cols(g, 1).start, MSG0[g])
        r0 = MSG0[g] + PAIR
        pay_v[r0:r0 + 16, :] = jnp.zeros((16, LANES), F32)
        for p in range(2):
            row = jnp.sum(sq_v[g, p], axis=0, keepdims=True)
            for c in range(3):
                pay_v[r0 + 3 * p + c:r0 + 3 * p + c + 1, :] = row[:, LANES * c:LANES * (c + 1)]

    def dgram(g):
        pack(do_v, g * GW, v_v, g * GW, MSG0[2 + g])

    held = {}

    def ar(m, k):
        half = MSG[m] // 2
        mine = pl.ds(pl.multiple_of(MSG0[m] + core * half, 8), half)
        theirs = pl.ds(pl.multiple_of(MSG0[m] + (1 - core) * half, 8), half)
        slot = pl.ds(MSG0[m] // 2, half)
        steps = ((pay_v.at[theirs], ar1.at[slot], partner), (pay_v.at[mine], ar2.at[slot], first),
                 (pay_v.at[mine], ar3.at[slot], second), (sum_v.at[mine], sum_v.at[mine], partner))

        def copy(n):
            src, dst, to = steps[n]
            return remote(src, dst, ar_send.at[m, n], ar_recv.at[m, n], to)
        if k:
            copy(k - 1).wait()
        if k == 1:
            pay_v[mine, :] = ar1[slot, :] + pay_v[mine, :]
        elif k == 2:
            pay_v[mine, :] = ar2[slot, :] + pay_v[mine, :]
        elif k == 3:
            sum_v[mine, :] = ar3[slot, :] + pay_v[mine, :]
        if k < 4:
            copy(k).start()

    def hook(*steps):
        def run():
            for m, k in steps:
                ar(m, k)
        return run

    def place(v, at, n):
        wide = jnp.concatenate([v, jnp.zeros((v.shape[0], n - LANES), v.dtype)], axis=1)
        return pltpu.roll(wide, at, 1) if at else wide

    def put(g, k, h, v):
        t, r = local(h)
        bd_v[g, k, t, r:r + HD, :] = place(v, r, TILE).astype(BF16)

    def head_block(base, h):
        r0 = base + HD * (h // 2)
        both = sum_v[r0:r0 + HD, :]
        if h % 2:
            both = pltpu.roll(both, LANES // 2, 1)
        return jnp.where(ok, both, 0.0)

    def sums(g, p):
        r0 = MSG0[g] + PAIR + 3 * p
        return jnp.concatenate([sum_v[r0 + c:r0 + c + 1, :] for c in range(3)], axis=1)

    def attn(g):
        sqrow = sums(g, 0)
        skwide = jnp.broadcast_to(sums(g, 1), (8, GW))
        for c in range(3):
            lanes = slice(LANES * c, LANES * (c + 1))
            row_v[g, lanes, :] = jnp.broadcast_to(sqrow[:, lanes], (LANES, LANES)).T
        for h in range(GH):
            hr = slice(HD * h, HD * (h + 1))
            skh = pltpu.roll(skwide, GW - HD * h, 1) if h else skwide
            skh = jnp.where(ok, jnp.broadcast_to(skh[:1, :LANES], (HD, LANES)), 1.0)
            den = jnp.sqrt(row_v[g, hr, :]) * jnp.sqrt(skh)
            cosine = head_block(MSG0[g], h) / den
            logit = jnp.where(ok, temp_ref[g * GH + h] * cosine, -jnp.inf)
            e = jnp.where(ok, jnp.exp(logit - jnp.max(logit, axis=1, keepdims=True)), 0.0)
            a = e / jnp.sum(e, axis=1, keepdims=True)
            for i, v in enumerate((a, cosine, den)):
                a_v[g, i, hr, :] = v
            put(g, 0, h, a)

    def attn_vjp(g):
        dsk = jnp.zeros((8, GW), F32)
        dtemp = jnp.zeros((1, LANES), F32)
        for h in range(GH):
            hr = slice(HD * h, HD * (h + 1))
            a, cosine, den = [a_v[g, i, hr, :] for i in range(3)]
            da = head_block(MSG0[2 + g], h)
            ds = a * (da - jnp.sum(a * da, axis=1, keepdims=True))
            dt = jnp.sum(jnp.sum(ds * cosine, axis=1, keepdims=True), axis=0, keepdims=True)
            dtemp = jnp.where(lane48[:1] == g * GH + h, dt, dtemp)
            dcos = temp_ref[g * GH + h] * ds
            w = dcos * cosine
            row_v[g, hr, :] = -jnp.sum(w, axis=1, keepdims=True) / row_v[g, hr, :]
            dsk = dsk - place(jnp.broadcast_to(jnp.sum(w, axis=0, keepdims=True), (8, LANES)), HD * h, GW)
            put(g, 1, h, dcos / den)
        dsq_v[g, 1] = dsk / sums(g, 1)
        dsq_v[g, 0] = jnp.concatenate([row_v[g, LANES * c:LANES * (c + 1), :].T[:8] for c in range(3)], axis=1)
        dtemp_out[:1, :] += dtemp

    def head_dot(g, x, k, c):
        lo = dot(x[:, :TILE], bd_v[g, k, 0], 1, c)
        hi = dot(x[:, LANES:], bd_v[g, k, 1], 1, c)
        return jnp.concatenate([lo[:, :LANES], lo[:, LANES:] + hi[:, :LANES], hi[:, LANES:]], axis=1)

    def heads_v(g):
        def body(b):
            rows = block(b, BIG)
            oc = slice(g * GW, (g + 1) * GW)
            qkv_v[rows, cols(g, 2)] = head_dot(g, do_v[rows, oc], 0, 0).astype(BF16)
            o = head_dot(g, v_v[rows, oc], 0, 1).astype(BF16)
            u_v[rows, oc] = o
            ot_v[oc, rows] = o.T
        loop(body, hi=ROWS // BIG)

    def heads_qk(g):
        def body(b):
            rows = block(b, BIG)
            q = qkv_v[rows, cols(g, 0)]
            k = qkv_v[rows, cols(g, 1)]
            dq = head_dot(g, k, 1, 1) + q.astype(F32) * dsq_v[g, 0, :1, :]
            dk = head_dot(g, q, 1, 0) + k.astype(F32) * dsq_v[g, 1, :1, :]
            qkv_v[rows, cols(g, 0)] = dq.astype(BF16)
            qkv_v[rows, cols(g, 1)] = dk.astype(BF16)
        loop(body, hi=ROWS // BIG)

    PART = ((0, 2), (1, 2), None, None, (0, 0), (0, 1), (1, 0), (1, 1))

    def s1(k, m):
        two = pl.ds(2 * m, 2)
        return remote(gw_v.at[k % SLOTS, two, 1 - core], r1.at[k, two], s1_send.at[k, m], s1_recv.at[k, m], partner)

    def gw_chunks(ch, n):
        def half(m, carry):
            mr = pl.ds(pl.multiple_of(m * GW, GW), GW)
            if PART[ch]:
                c0 = cols(*PART[ch]).start
                res = dot(ut_v[mr, :], qkv_v[:, c0:c0 + n * GW], 1, 0)
            else:
                res = dot(ot_v[mr, :], dy_v[...], 1, 0)
            for i in range(n):
                gw_v[(ch + i) % SLOTS, pl.ds(2 * m, 2)] = res[:, i * GW:(i + 1) * GW].reshape(2, 2, SHARD, GW)
            for i in range(n):
                s1(ch + i, m).start()
            return carry
        lax.fori_loop(0, 2, half, 0)

    def s2_copy(ch, b):
        return remote(r1.at[ch, chip(1 - ca, b)], r2.at[ch, b], s2_send.at[ch, b], s2_recv.at[ch, b], first)

    def s2_near(ch, b):
        i = chip(ca, b)
        r1[ch, i] += gw_v[ch % SLOTS, i, core]

    def s2_far(ch, b):
        i = chip(1 - ca, b)
        r1[ch, i] += gw_v[ch % SLOTS, i, core]
        s2_copy(ch, b).start()

    def s2(ch, last=False):
        for m in range(2):
            s1(ch, m).wait()
        s2_far(ch, 1 - cb)
        s2_near(ch, 1 - cb)
        if not last:
            s2_far(ch, cb)
            s2_near(ch, cb)

    def s3_copy(ch):
        return remote(r2.at[ch, 1 - cb], r3.at[ch], s3_send.at[ch], s3_recv.at[ch], second)

    def s3(ch):
        s2_copy(ch, 1 - cb).wait()
        r2[ch, 1 - cb] += r1[ch, chip(ca, 1 - cb)]
        s3_copy(ch).start()

    def s4(ch):
        s2_copy(ch, cb).wait()
        s3_copy(ch).wait()
        total = r3[ch] + (r2[ch, cb] + r1[ch, chip(ca, cb)])
        if PART[ch]:
            g, p = PART[ch]
            c0 = p * WIDTH + g * GW
            gwq_out[:, c0:c0 + GW] = total
        else:
            gwo_out[:, (ch - 2) * GW:(ch - 1) * GW] = total

    def out_tokens(b):
        rows = block(b)
        do_v[rows, :] = (x_v[rows, :].astype(F32) + dot(u_v[rows, :], wo_v[...], 1, 0)).astype(BF16)

    def final_dots(b):
        (du0, du1)[b % 2][...] = dot(qkv_v[b * BLK:(b + 1) * BLK, :], w_v[...], 1, 1)

    def final_norm(b):
        du_ref = (du0, du1)[b % 2]
        dgain = jnp.zeros((8, WIDTH), F32)
        dbias = jnp.zeros((8, WIDTH), F32)
        for i in range(0, BLK, LNR):
            sub = slice(b * BLK + i, b * BLK + i + LNR)
            xhat, rstd = normed_rows(b * BLK + i)
            du = du_ref[i:i + LNR, :]
            dgain = dgain + jnp.sum((du * xhat).reshape(-1, 8, WIDTH), axis=0)
            dbias = dbias + jnp.sum(du.reshape(-1, 8, WIDTH), axis=0)
            dxh = du * gain
            m1 = jnp.mean(dxh, axis=-1, keepdims=True)
            m2 = jnp.mean(dxh * xhat, axis=-1, keepdims=True)
            dx = rstd * (dxh - m1 - xhat * m2)
            x_v[sub, :] = (dy_v[sub, :].astype(F32) + dx).astype(BF16)
        gb_v[0] += dgain
        gb_v[1] += dbias

    def last_step(b):
        if b < NBLK:
            final_dots(b)
        if b:
            final_norm(b - 1)

    def gb_start():
        both = [jnp.sum(gb_v[i], axis=0, keepdims=True) for i in range(2)]
        gbs_v[0] = jnp.concatenate(both + [jnp.zeros((6, WIDTH), F32)], axis=0)
        c = remote(gbs_v.at[0], gbs_v.at[1], gb_send.at[3], gb_recv.at[3], partner)
        c.start()
        held['gb', 3] = c

    def gb_chips():
        held['gb', 3].wait()
        here = me // 2
        gbr_v[here] = gbs_v[0] + gbs_v[1]
        for k, to in enumerate((first, second, diagonal)):
            c = remote(gbr_v.at[here], gbr_v.at[here], gb_send.at[k], gb_recv.at[k], to)
            c.start()
            held['gb', k] = c

    def gb_end():
        for k in range(3):
            held['gb', k].wait()
        gb_out[...] = (gbr_v[0] + gbr_v[1]) + (gbr_v[2] + gbr_v[3])

    for ref in (sq_v, gb_v, dtemp_out, bd_v):
        ref[...] = jnp.zeros_like(ref)
    def first_step(b):
        if b + 1 < NBLK:
            for i in range(2):
                x_copy(2 * (b + 1) + i).wait()
            norm_block(b + 1)
        project(0, slice(b * BLK, (b + 1) * BLK))

    norm_block(0)
    for p in range(2):
        w_copy(0, p).wait()
    for b in range(NBLK):
        first_step(b)
    gram(0)
    pl.semaphore_wait(barrier, 4)
    ar(0, 0)
    for p in range(2):
        w_copy(1, p).wait()
    loop(lambda b: project(2, block(b, BIG)), ((0, hook((0, 1))),), hi=ROWS // BIG)
    gram(1)
    ar(1, 0)
    for g in range(2):
        w_copy(g, 2).wait()
    wo_copy.wait()
    for b in range(NBLK):
        dy_copy(b).wait()
    loop(values_and_do, ((0, hook((0, 2), (1, 1))), (2, hook((0, 3))), (3, hook((1, 2), (0, 4)))))
    attn(0)
    heads_v(0)
    ar(1, 3)
    gw_chunks(0, 1)
    dgram(0)
    ar(2, 0)
    ar(1, 4)
    attn(1)
    ar(2, 1)
    s2(0)
    heads_v(1)
    gw_chunks(1, 1)
    ar(2, 2)
    dgram(1)
    ar(3, 0)
    s2(1)
    ar(3, 1)
    s3(0)
    gw_chunks(2, 2)
    ar(2, 3)

    def mid():
        s2(2)
        s2(3)

    def late():
        ar(2, 4)
        s3(1)

    loop(out_tokens, ((0, mid), (1, late)), hi=NBLK - 1)
    attn_vjp(0)
    heads_qk(0)
    ar(3, 2)
    gw_chunks(4, 2)
    out_tokens(NBLK - 1)
    ar(3, 3)
    s2(4)
    s2(5)
    s3(2)
    ar(3, 4)
    attn_vjp(1)
    heads_qk(1)
    gw_chunks(6, 2)
    s3(3)
    last_step(0)
    s2(6, True)
    s2(7, True)
    s2_far(6, cb)
    s3(4)
    for b in range(1, NBLK + 1):
        last_step(b)
        if b in (2, 3):
            s3(3 + b)
    gb_start()
    for ch in range(4):
        s4(ch)
    gb_chips()
    s3(7)
    s2_far(7, cb)
    for ch in (6, 7):
        s2_near(ch, cb)
    for ch in (4, 5, 6):
        s4(ch)
    gb_end()
    s4(7)


def writer(out_v, gtok_v, gwq_v, gwo_v, gb_v, dtemp_v,
           out_hbm, gtok_hbm, gwq_hbm, gwo_hbm, gain_hbm, bias_hbm, dtemp_out, sem):
    pairs = [(gb_v.at[0], gain_hbm), (gb_v.at[1], bias_hbm), (gwo_v, gwo_hbm), (gwq_v, gwq_hbm)]
    for b in range(NBLK):
        rows = pl.ds(b * BLK, BLK)
        pairs += [(v.at[rows], hbm.at[rows]) for v, hbm in ((gtok_v, gtok_hbm), (out_v, out_hbm))]
    copies = [pltpu.make_async_copy(src, dst, sem.at[i]) for i, (src, dst) in enumerate(pairs)]
    for c in copies:
        c.start()
    dtemp_out[...] = dtemp_v[0, :HEADS]
    for c in copies:
        c.wait()


def block_step(x, dy, ln_gain, ln_bias, w_qkv, w_out, temperature):
    hbm = pl.BlockSpec(memory_space=pl.ANY)
    vmem = pl.BlockSpec(memory_space=pltpu.VMEM)
    smem = pl.BlockSpec(memory_space=pltpu.SMEM)
    dma = pltpu.SemaphoreType.DMA
    gtok, out, gwq, gwo, gb, dtemp = pl.pallas_call(
        kernel,
        out_shape=(
            pltpu.VMEM((ROWS, WIDTH), BF16),
            pltpu.VMEM((ROWS, WIDTH), BF16),
            pltpu.VMEM((SHARD, TOT), F32),
            pltpu.VMEM((SHARD, WIDTH), F32),
            pltpu.VMEM((8, WIDTH), F32),
            pltpu.VMEM((8, 128), F32),
        ),
        in_specs=[smem, vmem, vmem, hbm, hbm, hbm, hbm],
        out_specs=(vmem,) * 6,
        scratch_shapes=[
            pltpu.VMEM((ROWS, WIDTH), BF16),
            pltpu.VMEM((ROWS, WIDTH), BF16),
            pltpu.VMEM((WIDTH, ROWS), BF16),
            pltpu.VMEM((ROWS, TOT), BF16),
            pltpu.VMEM((ROWS, WIDTH), BF16),
            pltpu.VMEM((WIDTH, ROWS), BF16),
            pltpu.VMEM((WIDTH, TOT), BF16),
            pltpu.VMEM((WIDTH, WIDTH), BF16),
            pltpu.VMEM((2, TILE, TILE), F32),
            pltpu.VMEM((2, 2, 8, GW), F32),
            pltpu.VMEM((2, 3, GW, LANES), F32),
            pltpu.VMEM((2, 2, 2, TILE, TILE), BF16),
            pltpu.VMEM((2, 2, 8, GW), F32),
            pltpu.VMEM((2, GW, LANES), F32),
            pltpu.VMEM((PAY, LANES), F32),
            pltpu.VMEM((PAY // 2, LANES), F32),
            pltpu.VMEM((PAY // 2, LANES), F32),
            pltpu.VMEM((PAY // 2, LANES), F32),
            pltpu.VMEM((PAY, LANES), F32),
            pltpu.VMEM((SLOTS, 4, 2, SHARD, GW), F32),
            pltpu.VMEM((CHUNKS, 4, SHARD, GW), F32),
            pltpu.VMEM((CHUNKS, 2, SHARD, GW), F32),
            pltpu.VMEM((CHUNKS, SHARD, GW), F32),
            pltpu.VMEM((BLK, WIDTH), F32),
            pltpu.VMEM((BLK, WIDTH), F32),
            pltpu.VMEM((2, 8, WIDTH), F32),
            pltpu.VMEM((2, 8, WIDTH), F32),
            pltpu.VMEM((4, 8, WIDTH), F32),
            dma((NBLK,)), dma((7,)), dma((NFINE,)),
            dma((4, 4)), dma((4, 4)),
            dma((CHUNKS, 2)), dma((CHUNKS, 2)),
            dma((CHUNKS, 2)), dma((CHUNKS, 2)),
            dma((CHUNKS,)), dma((CHUNKS,)),
            dma((4,)), dma((4,)),
        ],
        compiler_params=pltpu.CompilerParams(
            collective_id=0, has_side_effects=True, vmem_limit_bytes=59400000),
    )(temperature, ln_gain, ln_bias, x, dy, w_qkv, w_out)
    return pl.pallas_call(
        writer,
        out_shape=(
            jax.ShapeDtypeStruct((ROWS, WIDTH), BF16),
            jax.ShapeDtypeStruct((ROWS, WIDTH), BF16),
            jax.ShapeDtypeStruct((SHARD, TOT), F32),
            jax.ShapeDtypeStruct((SHARD, WIDTH), F32),
            jax.ShapeDtypeStruct((WIDTH,), F32),
            jax.ShapeDtypeStruct((WIDTH,), F32),
            jax.ShapeDtypeStruct((HEADS,), F32),
        ),
        in_specs=[vmem] * 6,
        out_specs=(hbm,) * 6 + (vmem,),
        scratch_shapes=[dma((4 + 2 * NBLK,))],
        compiler_params=pltpu.CompilerParams(vmem_limit_bytes=1000000),
    )(out, gtok, gwq, gwo, gb, dtemp)


def solution(mesh):
    row_spec = P(('dp', 'sp'), None)
    part_spec = P('dp')
    full_spec = P()

    return jax.shard_map(block_step, mesh=mesh,
                         in_specs=(row_spec, row_spec, full_spec, full_spec, full_spec, full_spec, full_spec),
                         out_specs=(row_spec, row_spec, row_spec, row_spec, part_spec, part_spec, part_spec),
                         check_vma=False)
```

```python
import jax
import jax.numpy as jnp
from jax import lax
from jax.experimental import pallas as pl
from jax.experimental.pallas import tpu as pltpu
from jax.sharding import PartitionSpec as P

F32 = jnp.float32
BF16 = jnp.bfloat16
MESH = pl.DeviceIdType.MESH

ROWS = 2048
WIDTH = 768
HEADS = 16
HD = 48
GW = 384
GH = 8
BLK = 512
NBLK = ROWS // BLK
BIG = 1024
FINE = 256
NFINE = ROWS // FINE
LNR = 16
PAIR = 192
TOT = 2304
LANES = 128
TILE = 256
SPLIT = 5
MSG = (208, 208, 192, 192)
MSG0 = (0, 208, 416, 608)
PAY = 800
SLOTS = 4
ORDER = ((0, 1, 2), (4, 5, 3))
SHARD = 96
CHUNKS = 8


def dot(a, b, ca, cb):
    return lax.dot_general(a, b, (((ca,), (cb,)), ((), ())), preferred_element_type=F32)


def kernel(temp_ref, gain_ref, bias_ref, x_hbm, dy_hbm, wqkv_hbm, wout_hbm,
           x_v, do_v, gwq_out, gwo_out, gb_out, dtemp_out,
           dy_v, u_v, ut_v, qkv_v, v_v, ot_v, w_v, wo_v,
           gm_v, sq_v, a_v, bd_v, dsq_v, row_v, pay_v, ar1, ar2, ar3, sum_v,
           gw_v, r1, r2, r3, du0, du1, gb_v, gbs_v, gbr_v,
           in_sem, w_sem, x_sem,
           ar_send, ar_recv, s1_send, s1_recv, s2_send, s2_recv, s3_send, s3_recv, gb_send, gb_recv):
    dp = lax.axis_index('dp')
    me = lax.axis_index('sp')
    core = me % 2
    cx = (me // 2) % 2
    cy = me // 4
    partner = me + 1 - 2 * core
    xn = me + 2 - 4 * cx
    yn = me + 4 - 8 * cy
    first = xn + core * (yn - xn)
    second = yn + core * (xn - yn)
    diagonal = xn + 4 - 8 * cy
    ca = cx + core * (cy - cx)
    cb = cy + core * (cx - cy)

    def chip(a, b):
        return a * (1 + core) + b * (2 - core)

    def dev(i):
        return (dp, i)

    def remote(src, dst, ss, rs, to):
        return pltpu.make_async_remote_copy(src_ref=src, dst_ref=dst, send_sem=ss, recv_sem=rs,
                                            device_id=dev(to), device_id_type=MESH)

    barrier = pltpu.get_barrier_semaphore()
    for peer in (partner, xn, yn, diagonal):
        pl.semaphore_signal(barrier, inc=1, device_id=dev(peer), device_id_type=MESH)

    def cols(g, p):
        return slice(ORDER[g][p] * GW, (ORDER[g][p] + 1) * GW)

    def w_copy(g, p):
        return pltpu.make_async_copy(wqkv_hbm.at[:, pl.ds(p * WIDTH + g * GW, GW)],
                                     w_v.at[:, pl.ds(ORDER[g][p] * GW, GW)], w_sem.at[ORDER[g][p]])

    wo_copy = pltpu.make_async_copy(wout_hbm, wo_v, w_sem.at[6])

    def x_copy(b):
        rows = pl.ds(b * FINE, FINE)
        return pltpu.make_async_copy(x_hbm.at[rows], x_v.at[rows], x_sem.at[b])

    def dy_copy(b):
        rows = pl.ds(b * BLK, BLK)
        return pltpu.make_async_copy(dy_hbm.at[rows], dy_v.at[rows], in_sem.at[b])

    for b in range(2):
        x_copy(b).start()
    for p in range(2):
        w_copy(0, p).start()
    for b in range(2, NFINE):
        x_copy(b).start()
    for p in range(2):
        w_copy(1, p).start()
    for g in range(2):
        w_copy(g, 2).start()
    wo_copy.start()
    for b in range(NBLK):
        dy_copy(b).start()

    gain = gain_ref[...].reshape(1, WIDTH)
    bias = bias_ref[...].reshape(1, WIDTH)

    def loop(f, hooks=(), lo=0, hi=NBLK):
        def body(b, carry):
            f(b)
            for at, hook in hooks:
                pl.when(b == at)(hook)
            return carry
        lax.fori_loop(lo, hi, body, 0)

    def block(b, n=BLK):
        return pl.ds(pl.multiple_of(b * n, n), n)

    def normed_rows(r0):
        xf = x_v[pl.ds(r0, LNR), :].astype(F32)
        c = xf - jnp.mean(xf, axis=-1, keepdims=True)
        rstd = lax.rsqrt(jnp.mean(c * c, axis=-1, keepdims=True) + 1e-6)
        return c * rstd, rstd

    def norm_block(b):
        for r0 in range(b * BLK, (b + 1) * BLK, LNR):
            if b == 0 and r0 % FINE == 0:
                x_copy(r0 // FINE).wait()
            xhat, _ = normed_rows(r0)
            u_v[r0:r0 + LNR, :] = (xhat * gain + bias).astype(BF16)

    def sumsq(v):
        vf = v.astype(F32)
        return jnp.sum((vf * vf).reshape(-1, 8, GW), axis=0)

    def project(n, rows):
        c = slice(n * WIDTH, (n + 1) * WIDTH)
        res = dot(u_v[rows, :], w_v[:, c], 1, 0).astype(BF16)
        if n == 1:
            v_v[rows, :] = res
        else:
            qkv_v[rows, c] = res
            sq_v[n // 2, 0] += sumsq(res[:, :GW])
            sq_v[n // 2, 1] += sumsq(res[:, GW:])

    def values_and_do(b):
        rows = block(b)
        project(1, rows)
        do_v[rows, :] = dot(dy_v[rows, :], wo_v[...], 1, 1).astype(BF16)
        ut_v[:, rows] = u_v[rows, :].T

    lane48 = lax.broadcasted_iota(jnp.int32, (HD, LANES), 1)
    ok = lane48 < HD

    def local(h):
        t = int(h >= SPLIT)
        return t, HD * h - LANES * t

    def pack(left, lc, right, rc, base):
        for t in range(2):
            off = LANES * t
            gm_v[t] = dot(left[:, lc + off:lc + off + TILE], right[:, rc + off:rc + off + TILE], 0, 0)

        def piece(h, to):
            t, r = local(h)
            lo = r // LANES * LANES
            n = LANES if r + HD <= lo + LANES else TILE
            v = gm_v[t, r:r + HD, lo:lo + n]
            move = (to - (r - lo)) % n
            if move:
                v = pltpu.roll(v, move, 1)
            return v[:, :LANES]
        for p in range(GH // 2):
            a = piece(2 * p, 0)
            d = piece(2 * p + 1, LANES // 2)
            side = lane48 - LANES // 2
            both = jnp.where(ok, a, jnp.where((side >= 0) & (side < HD), d, 0.0))
            pay_v[base + HD * p:base + HD * (p + 1), :] = both

    def gram(g):
        pack(qkv_v, cols(g, 0).start, qkv_v, cols(g, 1).start, MSG0[g])
        r0 = MSG0[g] + PAIR
        pay_v[r0:r0 + 16, :] = jnp.zeros((16, LANES), F32)
        for p in range(2):
            row = jnp.sum(sq_v[g, p], axis=0, keepdims=True)
            for c in range(3):
                pay_v[r0 + 3 * p + c:r0 + 3 * p + c + 1, :] = row[:, LANES * c:LANES * (c + 1)]

    def dgram(g):
        pack(do_v, g * GW, v_v, g * GW, MSG0[2 + g])

    held = {}

    def ar(m, k):
        half = MSG[m] // 2
        mine = pl.ds(pl.multiple_of(MSG0[m] + core * half, 8), half)
        theirs = pl.ds(pl.multiple_of(MSG0[m] + (1 - core) * half, 8), half)
        slot = pl.ds(MSG0[m] // 2, half)
        steps = ((pay_v.at[theirs], ar1.at[slot], partner), (pay_v.at[mine], ar2.at[slot], first),
                 (pay_v.at[mine], ar3.at[slot], second), (sum_v.at[mine], sum_v.at[mine], partner))

        def copy(n):
            src, dst, to = steps[n]
            return remote(src, dst, ar_send.at[m, n], ar_recv.at[m, n], to)
        if k:
            copy(k - 1).wait()
        if k == 1:
            pay_v[mine, :] = ar1[slot, :] + pay_v[mine, :]
        elif k == 2:
            pay_v[mine, :] = ar2[slot, :] + pay_v[mine, :]
        elif k == 3:
            sum_v[mine, :] = ar3[slot, :] + pay_v[mine, :]
        if k < 4:
            copy(k).start()

    def hook(*steps):
        def run():
            for m, k in steps:
                ar(m, k)
        return run

    def place(v, at, n):
        wide = jnp.concatenate([v, jnp.zeros((v.shape[0], n - LANES), v.dtype)], axis=1)
        return pltpu.roll(wide, at, 1) if at else wide

    def put(g, k, h, v):
        t, r = local(h)
        bd_v[g, k, t, r:r + HD, :] = place(v, r, TILE).astype(BF16)

    def head_block(base, h):
        r0 = base + HD * (h // 2)
        both = sum_v[r0:r0 + HD, :]
        if h % 2:
            both = pltpu.roll(both, LANES // 2, 1)
        return jnp.where(ok, both, 0.0)

    def sums(g, p):
        r0 = MSG0[g] + PAIR + 3 * p
        return jnp.concatenate([sum_v[r0 + c:r0 + c + 1, :] for c in range(3)], axis=1)

    def attn(g):
        sqrow = sums(g, 0)
        skwide = jnp.broadcast_to(sums(g, 1), (8, GW))
        for c in range(3):
            lanes = slice(LANES * c, LANES * (c + 1))
            row_v[g, lanes, :] = jnp.broadcast_to(sqrow[:, lanes], (LANES, LANES)).T
        for h in range(GH):
            hr = slice(HD * h, HD * (h + 1))
            skh = pltpu.roll(skwide, GW - HD * h, 1) if h else skwide
            skh = jnp.where(ok, jnp.broadcast_to(skh[:1, :LANES], (HD, LANES)), 1.0)
            den = jnp.sqrt(row_v[g, hr, :]) * jnp.sqrt(skh)
            cosine = head_block(MSG0[g], h) / den
            logit = jnp.where(ok, temp_ref[g * GH + h] * cosine, -jnp.inf)
            e = jnp.where(ok, jnp.exp(logit - jnp.max(logit, axis=1, keepdims=True)), 0.0)
            a = e / jnp.sum(e, axis=1, keepdims=True)
            for i, v in enumerate((a, cosine, den)):
                a_v[g, i, hr, :] = v
            put(g, 0, h, a)

    def attn_vjp(g):
        dsk = jnp.zeros((8, GW), F32)
        dtemp = jnp.zeros((1, LANES), F32)
        for h in range(GH):
            hr = slice(HD * h, HD * (h + 1))
            a, cosine, den = [a_v[g, i, hr, :] for i in range(3)]
            da = head_block(MSG0[2 + g], h)
            ds = a * (da - jnp.sum(a * da, axis=1, keepdims=True))
            dt = jnp.sum(jnp.sum(ds * cosine, axis=1, keepdims=True), axis=0, keepdims=True)
            dtemp = jnp.where(lane48[:1] == g * GH + h, dt, dtemp)
            dcos = temp_ref[g * GH + h] * ds
            w = dcos * cosine
            row_v[g, hr, :] = -jnp.sum(w, axis=1, keepdims=True) / row_v[g, hr, :]
            dsk = dsk - place(jnp.broadcast_to(jnp.sum(w, axis=0, keepdims=True), (8, LANES)), HD * h, GW)
            put(g, 1, h, dcos / den)
        dsq_v[g, 1] = dsk / sums(g, 1)
        dsq_v[g, 0] = jnp.concatenate([row_v[g, LANES * c:LANES * (c + 1), :].T[:8] for c in range(3)], axis=1)
        dtemp_out[:1, :] += dtemp

    def head_dot(g, x, k, c):
        lo = dot(x[:, :TILE], bd_v[g, k, 0], 1, c)
        hi = dot(x[:, LANES:], bd_v[g, k, 1], 1, c)
        return jnp.concatenate([lo[:, :LANES], lo[:, LANES:] + hi[:, :LANES], hi[:, LANES:]], axis=1)

    def heads_v(g):
        def body(b):
            rows = block(b, BIG)
            oc = slice(g * GW, (g + 1) * GW)
            qkv_v[rows, cols(g, 2)] = head_dot(g, do_v[rows, oc], 0, 0).astype(BF16)
            o = head_dot(g, v_v[rows, oc], 0, 1).astype(BF16)
            u_v[rows, oc] = o
            ot_v[oc, rows] = o.T
        loop(body, hi=ROWS // BIG)

    def heads_qk(g):
        def body(b):
            rows = block(b, BIG)
            q = qkv_v[rows, cols(g, 0)]
            k = qkv_v[rows, cols(g, 1)]
            dq = head_dot(g, k, 1, 1) + q.astype(F32) * dsq_v[g, 0, :1, :]
            dk = head_dot(g, q, 1, 0) + k.astype(F32) * dsq_v[g, 1, :1, :]
            qkv_v[rows, cols(g, 0)] = dq.astype(BF16)
            qkv_v[rows, cols(g, 1)] = dk.astype(BF16)
        loop(body, hi=ROWS // BIG)

    PART = ((0, 2), (1, 2), None, None, (0, 0), (0, 1), (1, 0), (1, 1))

    def s1(k, m):
        two = pl.ds(2 * m, 2)
        return remote(gw_v.at[k % SLOTS, two, 1 - core], r1.at[k, two], s1_send.at[k, m], s1_recv.at[k, m], partner)

    def gw_chunks(ch, n):
        def half(m, carry):
            mr = pl.ds(pl.multiple_of(m * GW, GW), GW)
            if PART[ch]:
                c0 = cols(*PART[ch]).start
                res = dot(ut_v[mr, :], qkv_v[:, c0:c0 + n * GW], 1, 0)
            else:
                res = dot(ot_v[mr, :], dy_v[...], 1, 0)
            for i in range(n):
                gw_v[(ch + i) % SLOTS, pl.ds(2 * m, 2)] = res[:, i * GW:(i + 1) * GW].reshape(2, 2, SHARD, GW)
            for i in range(n):
                s1(ch + i, m).start()
            return carry
        lax.fori_loop(0, 2, half, 0)

    def s2_copy(ch, b):
        return remote(r1.at[ch, chip(1 - ca, b)], r2.at[ch, b], s2_send.at[ch, b], s2_recv.at[ch, b], first)

    def s2_near(ch, b):
        i = chip(ca, b)
        r1[ch, i] += gw_v[ch % SLOTS, i, core]

    def s2_far(ch, b):
        i = chip(1 - ca, b)
        r1[ch, i] += gw_v[ch % SLOTS, i, core]
        s2_copy(ch, b).start()

    def s2(ch, last=False):
        for m in range(2):
            s1(ch, m).wait()
        s2_far(ch, 1 - cb)
        s2_near(ch, 1 - cb)
        if not last:
            s2_far(ch, cb)
            s2_near(ch, cb)

    def s3_copy(ch):
        return remote(r2.at[ch, 1 - cb], r3.at[ch], s3_send.at[ch], s3_recv.at[ch], second)

    def s3(ch):
        s2_copy(ch, 1 - cb).wait()
        r2[ch, 1 - cb] += r1[ch, chip(ca, 1 - cb)]
        s3_copy(ch).start()

    def s4(ch):
        s2_copy(ch, cb).wait()
        s3_copy(ch).wait()
        total = r3[ch] + (r2[ch, cb] + r1[ch, chip(ca, cb)])
        if PART[ch]:
            g, p = PART[ch]
            c0 = p * WIDTH + g * GW
            gwq_out[:, c0:c0 + GW] = total
        else:
            gwo_out[:, (ch - 2) * GW:(ch - 1) * GW] = total

    def out_tokens(b):
        rows = block(b)
        do_v[rows, :] = (x_v[rows, :].astype(F32) + dot(u_v[rows, :], wo_v[...], 1, 0)).astype(BF16)

    def final_dots(b):
        (du0, du1)[b % 2][...] = dot(qkv_v[b * BLK:(b + 1) * BLK, :], w_v[...], 1, 1)

    def final_norm(b):
        du_ref = (du0, du1)[b % 2]
        dgain = jnp.zeros((8, WIDTH), F32)
        dbias = jnp.zeros((8, WIDTH), F32)
        for i in range(0, BLK, LNR):
            sub = slice(b * BLK + i, b * BLK + i + LNR)
            xhat, rstd = normed_rows(b * BLK + i)
            du = du_ref[i:i + LNR, :]
            dgain = dgain + jnp.sum((du * xhat).reshape(-1, 8, WIDTH), axis=0)
            dbias = dbias + jnp.sum(du.reshape(-1, 8, WIDTH), axis=0)
            dxh = du * gain
            m1 = jnp.mean(dxh, axis=-1, keepdims=True)
            m2 = jnp.mean(dxh * xhat, axis=-1, keepdims=True)
            dx = rstd * (dxh - m1 - xhat * m2)
            x_v[sub, :] = (dy_v[sub, :].astype(F32) + dx).astype(BF16)
        gb_v[0] += dgain
        gb_v[1] += dbias

    def last_step(b):
        if b < NBLK:
            final_dots(b)
        if b:
            final_norm(b - 1)

    def gb_start():
        both = [jnp.sum(gb_v[i], axis=0, keepdims=True) for i in range(2)]
        gbs_v[0] = jnp.concatenate(both + [jnp.zeros((6, WIDTH), F32)], axis=0)
        c = remote(gbs_v.at[0], gbs_v.at[1], gb_send.at[3], gb_recv.at[3], partner)
        c.start()
        held['gb', 3] = c

    def gb_chips():
        held['gb', 3].wait()
        here = me // 2
        gbr_v[here] = gbs_v[0] + gbs_v[1]
        for k, to in enumerate((first, second, diagonal)):
            c = remote(gbr_v.at[here], gbr_v.at[here], gb_send.at[k], gb_recv.at[k], to)
            c.start()
            held['gb', k] = c

    def gb_end():
        for k in range(3):
            held['gb', k].wait()
        gb_out[...] = (gbr_v[0] + gbr_v[1]) + (gbr_v[2] + gbr_v[3])

    for ref in (sq_v, gb_v, dtemp_out, bd_v):
        ref[...] = jnp.zeros_like(ref)
    def first_step(b):
        if b + 1 < NBLK:
            for i in range(2):
                x_copy(2 * (b + 1) + i).wait()
            norm_block(b + 1)
        project(0, slice(b * BLK, (b + 1) * BLK))

    norm_block(0)
    for p in range(2):
        w_copy(0, p).wait()
    for b in range(NBLK):
        first_step(b)
    gram(0)
    pl.semaphore_wait(barrier, 4)
    ar(0, 0)
    for p in range(2):
        w_copy(1, p).wait()
    loop(lambda b: project(2, block(b, BIG)), ((0, hook((0, 1))),), hi=ROWS // BIG)
    gram(1)
    ar(1, 0)
    for g in range(2):
        w_copy(g, 2).wait()
    wo_copy.wait()
    for b in range(NBLK):
        dy_copy(b).wait()
    loop(values_and_do, ((0, hook((0, 2), (1, 1))), (2, hook((0, 3))), (3, hook((1, 2), (0, 4)))))
    attn(0)
    heads_v(0)
    ar(1, 3)
    gw_chunks(0, 1)
    dgram(0)
    ar(2, 0)
    ar(1, 4)
    attn(1)
    ar(2, 1)
    s2(0)
    heads_v(1)
    gw_chunks(1, 1)
    ar(2, 2)
    dgram(1)
    ar(3, 0)
    s2(1)
    ar(3, 1)
    s3(0)
    gw_chunks(2, 2)
    ar(2, 3)

    def mid():
        s2(2)
        s2(3)

    def late():
        ar(2, 4)
        s3(1)

    loop(out_tokens, ((0, mid), (1, late)), hi=NBLK - 1)
    attn_vjp(0)
    heads_qk(0)
    ar(3, 2)
    gw_chunks(4, 2)
    out_tokens(NBLK - 1)
    ar(3, 3)
    s2(4)
    s2(5)
    s3(2)
    ar(3, 4)
    attn_vjp(1)
    heads_qk(1)
    gw_chunks(6, 2)
    s3(3)
    last_step(0)
    s2(6, True)
    s2(7, True)
    s2_far(6, cb)
    s3(4)
    for b in range(1, NBLK + 1):
        last_step(b)
        if b in (2, 3):
            s3(3 + b)
    gb_start()
    for ch in range(4):
        s4(ch)
    gb_chips()
    s3(7)
    s2_far(7, cb)
    for ch in (6, 7):
        s2_near(ch, cb)
    for ch in (4, 5, 6):
        s4(ch)
    gb_end()
    s4(7)


def writer(out_v, gtok_v, gwq_v, gwo_v, gb_v, dtemp_v,
           out_hbm, gtok_hbm, gwq_hbm, gwo_hbm, gain_hbm, bias_hbm, dtemp_out, sem):
    pairs = [(gb_v.at[0], gain_hbm), (gb_v.at[1], bias_hbm), (gwo_v, gwo_hbm), (gwq_v, gwq_hbm)]
    for b in range(NBLK):
        rows = pl.ds(b * BLK, BLK)
        pairs += [(v.at[rows], hbm.at[rows]) for v, hbm in ((gtok_v, gtok_hbm), (out_v, out_hbm))]
    copies = [pltpu.make_async_copy(src, dst, sem.at[i]) for i, (src, dst) in enumerate(pairs)]
    for c in copies:
        c.start()
    dtemp_out[...] = dtemp_v[0, :HEADS]
    for c in copies:
        c.wait()


def block_step(x, dy, ln_gain, ln_bias, w_qkv, w_out, temperature):
    hbm = pl.BlockSpec(memory_space=pl.ANY)
    vmem = pl.BlockSpec(memory_space=pltpu.VMEM)
    smem = pl.BlockSpec(memory_space=pltpu.SMEM)
    dma = pltpu.SemaphoreType.DMA
    gtok, out, gwq, gwo, gb, dtemp = pl.pallas_call(
        kernel,
        out_shape=(
            pltpu.VMEM((ROWS, WIDTH), BF16),
            pltpu.VMEM((ROWS, WIDTH), BF16),
            pltpu.VMEM((SHARD, TOT), F32),
            pltpu.VMEM((SHARD, WIDTH), F32),
            pltpu.VMEM((8, WIDTH), F32),
            pltpu.VMEM((8, 128), F32),
        ),
        in_specs=[smem, vmem, vmem, hbm, hbm, hbm, hbm],
        out_specs=(vmem,) * 6,
        scratch_shapes=[
            pltpu.VMEM((ROWS, WIDTH), BF16),
            pltpu.VMEM((ROWS, WIDTH), BF16),
            pltpu.VMEM((WIDTH, ROWS), BF16),
            pltpu.VMEM((ROWS, TOT), BF16),
            pltpu.VMEM((ROWS, WIDTH), BF16),
            pltpu.VMEM((WIDTH, ROWS), BF16),
            pltpu.VMEM((WIDTH, TOT), BF16),
            pltpu.VMEM((WIDTH, WIDTH), BF16),
            pltpu.VMEM((2, TILE, TILE), F32),
            pltpu.VMEM((2, 2, 8, GW), F32),
            pltpu.VMEM((2, 3, GW, LANES), F32),
            pltpu.VMEM((2, 2, 2, TILE, TILE), BF16),
            pltpu.VMEM((2, 2, 8, GW), F32),
            pltpu.VMEM((2, GW, LANES), F32),
            pltpu.VMEM((PAY, LANES), F32),
            pltpu.VMEM((PAY // 2, LANES), F32),
            pltpu.VMEM((PAY // 2, LANES), F32),
            pltpu.VMEM((PAY // 2, LANES), F32),
            pltpu.VMEM((PAY, LANES), F32),
            pltpu.VMEM((SLOTS, 4, 2, SHARD, GW), F32),
            pltpu.VMEM((CHUNKS, 4, SHARD, GW), F32),
            pltpu.VMEM((CHUNKS, 2, SHARD, GW), F32),
            pltpu.VMEM((CHUNKS, SHARD, GW), F32),
            pltpu.VMEM((BLK, WIDTH), F32),
            pltpu.VMEM((BLK, WIDTH), F32),
            pltpu.VMEM((2, 8, WIDTH), F32),
            pltpu.VMEM((2, 8, WIDTH), F32),
            pltpu.VMEM((4, 8, WIDTH), F32),
            dma((NBLK,)), dma((7,)), dma((NFINE,)),
            dma((4, 4)), dma((4, 4)),
            dma((CHUNKS, 2)), dma((CHUNKS, 2)),
            dma((CHUNKS, 2)), dma((CHUNKS, 2)),
            dma((CHUNKS,)), dma((CHUNKS,)),
            dma((4,)), dma((4,)),
        ],
        compiler_params=pltpu.CompilerParams(
            collective_id=0, has_side_effects=True, vmem_limit_bytes=59400000),
    )(temperature, ln_gain, ln_bias, x, dy, w_qkv, w_out)
    return pl.pallas_call(
        writer,
        out_shape=(
            jax.ShapeDtypeStruct((ROWS, WIDTH), BF16),
            jax.ShapeDtypeStruct((ROWS, WIDTH), BF16),
            jax.ShapeDtypeStruct((SHARD, TOT), F32),
            jax.ShapeDtypeStruct((SHARD, WIDTH), F32),
            jax.ShapeDtypeStruct((WIDTH,), F32),
            jax.ShapeDtypeStruct((WIDTH,), F32),
            jax.ShapeDtypeStruct((HEADS,), F32),
        ),
        in_specs=[vmem] * 6,
        out_specs=(hbm,) * 6 + (vmem,),
        scratch_shapes=[dma((4 + 2 * NBLK,))],
        compiler_params=pltpu.CompilerParams(vmem_limit_bytes=1000000),
    )(out, gtok, gwq, gwo, gb, dtemp)


def solution(mesh):
    row_spec = P(('dp', 'sp'), None)
    part_spec = P('dp')
    full_spec = P()

    return jax.shard_map(block_step, mesh=mesh,
                         in_specs=(row_spec, row_spec, full_spec, full_spec, full_spec, full_spec, full_spec),
                         out_specs=(row_spec, row_spec, row_spec, row_spec, part_spec, part_spec, part_spec),
                         check_vma=False)
```
